32 devices in a mesh: job: 2 (over y), aux: 16 (over z, x, core).
Axes of the slice: x: 2, y: 2, z: 4, core: 2. Of those that a mesh axis runs over, the one named last changes fastest.
Arguments:
- ints_ov: bfloat16 [256, 384, 384], P(('job', 'aux')), parts along dimension 0, may hold values from -0.3125 to 0.3125
- ints_oo: bfloat16 [256, 2, 384], P(('job', 'aux')), parts along dimension 0, may hold values from -1.5 to 1.5
- trial: bfloat16 [64, 4, 384], P('job'), parts along dimension 0, may hold values from -6 to 6
- occ_energy: float32 [64], P('job'), parts along dimension 0, may hold values from -1 to -0.2
- vir_energy: float32 [32000], P('job'), parts along dimension 0, may hold values from 0.2 to 2.5
- root_shift: float32 [8], P('job'), parts along dimension 0, may hold values from 0.1 to 0.6
- vir_blocks: int32 [32, 3], P('job'), parts along dimension 0, may hold values from 0 to 124, as said below
- pair_list: int32 [32, 4, 2], P('job'), parts along dimension 0, may hold values from 0 to 31, as said below
- pair_count: int32 [32], P('job'), parts along dimension 0, may hold values from 2 to 4, as said below
Outputs:
- sigma: float32 [64, 4, 384], P(('job', 'aux')), parts along dimension 0
The draws below stay inside these ranges and needn't reach their ends.
There are 2 independent parts, one for each index of `job`. The reference program is written for one: setup_inputs(seed, part) draws one part's arguments, and reference() takes and returns one part's arrays. A program takes and returns all parts, laid end to end along the dimension named above; each array names one. Nothing has to cross between parts.
Inputs may be any that keep to these rules, and one draw needn't show every extreme that they name: `pair_count`: some domain has 4 live pairs. `pair_list`: for domain d all 4 slots hold distinct pairs (i, j): i an occupied of domain d (d * 2 to d * 2 + 1) and j an occupied of one of the domains d + 1 to d + 3, taken cyclically modulo 16; slots from pair_count[d] on are not live. `vir_blocks`: the blocks of one domain are distinct.
All inputs are finite; a program needn't handle non-finite values.
Results may differ from the reference program's by a relative error of at most 0.00036.
Values may be sent and summed in bfloat16 or wider, within the bound.
A program may use at most 128 MiB of HBM per device.

```python
import math
import jax
import jax.numpy as jnp
from jax import lax

FB = 384
DV = 384
NV = 16000
K = 4
OD = 2
NN = 4
PMAX = 4
NDOM = 16
OCC = 32
SLAB = 8


def pair_tables(key):
    base_key = jax.random.fold_in(key, 7001)
    uniform_ints = jax.random.randint(jax.random.fold_in(base_key, 1), (NDOM,), 0, 16)
    counts = 2 + (uniform_ints >= 10).astype(jnp.int32) + (uniform_ints >= 14).astype(jnp.int32)
    counts = jnp.minimum(counts, PMAX)
    busiest = jax.random.randint(jax.random.fold_in(base_key, 2), (), 0, NDOM)
    domains = jnp.arange(NDOM, dtype=jnp.int32)
    counts = jnp.where(domains == busiest, PMAX, counts).astype(jnp.int32)
    options = OD * OD * (NN - 1)
    domain_keys = jax.random.split(jax.random.fold_in(base_key, 3), NDOM)
    chosen = jax.vmap(lambda one_key: jax.random.permutation(one_key, options)[:PMAX])(domain_keys).astype(jnp.int32)
    per_side = (NN - 1) * OD
    own_slot = chosen // per_side
    remainder = chosen % per_side
    ahead_by = 1 + remainder // OD
    other_slot = remainder % OD
    occ_first = domains[:, None] * OD + own_slot
    occ_second = (domains[:, None] + ahead_by) % NDOM * OD + other_slot
    return (counts, jnp.stack([occ_first, occ_second], axis=-1).astype(jnp.int32))


def draw_pair_list(key, part):
    return pair_tables(key)[1]


def draw_pair_count(key, part):
    return pair_tables(key)[0]


def draw_vir_blocks(key, part):
    domain_keys = jax.random.split(jax.random.fold_in(key, 9001), NDOM)
    chosen = jax.vmap(lambda one_key: jax.random.permutation(one_key, NV // 128)[:DV // 128])(domain_keys)
    return chosen.astype(jnp.int32)


def block_levels(own_key, shape, cuts, least, largest):
    gain, own = 1.0, jax.random.fold_in(own_key, 6)
    for axis_at, blocks in cuts:
        heights = jnp.exp(jax.random.uniform(jax.random.fold_in(own, axis_at), (blocks,), jnp.float32, least / len(cuts), largest / len(cuts)))
        gain = gain * jnp.repeat(heights, shape[axis_at] // blocks).reshape([-1 if axis == axis_at else 1 for axis in range(len(shape))])
    return gain


def noise(key, shape, width, most, shards=(), kind=jnp.bfloat16):
    factor_of = block_levels(key, shape, shards, -0.22, 0.18) if shards else 1.0
    array = jax.random.normal(key, shape, jnp.float32) * width * factor_of
    return jnp.minimum(jnp.maximum(array, -most), most).astype(kind)


def setup_inputs(seed: int = 0, part: int = 0) -> dict:
    arg_keys = jax.random.split(jax.random.key(seed), 10)
    own_keys = jax.random.split(jax.random.fold_in(arg_keys[9], part), 10)
    ints_ov = noise(own_keys[0], (NDOM * SLAB, FB, DV), FB ** -0.5, 0.3125, ((0, 16),))
    ints_oo = noise(own_keys[1], (NDOM * SLAB, OD, FB), 0.25, 1.5, ((0, 16),))
    trial = noise(own_keys[2], (OCC, K, DV), 1.0, 6.0)
    occ_energy = jnp.clip(jax.random.uniform(own_keys[3], (OCC,), jnp.float32, -1.0, -0.2), -1.0, -0.2)
    vir_energy = jnp.clip(jnp.exp(jax.random.uniform(own_keys[4], (NV,), jnp.float32, math.log(0.2), math.log(2.5))), 0.2, 2.5)
    root_shift = jnp.clip(jax.random.uniform(own_keys[5], (K,), jnp.float32, 0.1, 0.6), 0.1, 0.6)
    vir_blocks = draw_vir_blocks(jax.random.fold_in(jax.random.fold_in(arg_keys[9], part), 71), part)
    pair_list = draw_pair_list(jax.random.fold_in(jax.random.fold_in(arg_keys[9], part), 71), part)
    pair_count = draw_pair_count(jax.random.fold_in(jax.random.fold_in(arg_keys[9], part), 71), part)
    return dict(ints_ov=ints_ov, ints_oo=ints_oo, trial=trial, occ_energy=occ_energy, vir_energy=vir_energy, root_shift=root_shift, vir_blocks=vir_blocks, pair_list=pair_list, pair_count=pair_count)


def product(pattern, left_arg, right_arg):
    return jnp.einsum(pattern, left_arg.astype(jnp.float32), right_arg.astype(jnp.float32))


def reference(ints_ov, ints_oo, trial, occ_energy, vir_energy, root_shift, vir_blocks, pair_list, pair_count):
    slab_table = ints_ov.reshape(NDOM, SLAB, FB, DV)
    coupling_table = ints_oo.reshape(NDOM, SLAB, OD, FB)
    level_table = vir_energy.reshape(NV // 128, 128)

    def levels(domain):
        return jnp.take(level_table, vir_blocks[domain], axis=0).reshape(DV)

    def dressed(coupling, domain):
        occupied = lax.dynamic_slice_in_dim(trial, (domain * OD).astype(jnp.int32), OD, 0)
        return (-product("lq,lka->kqa", coupling, occupied)).astype(jnp.bfloat16)

    def deposit(accum_sigma, contribution, domain):
        start_row = (domain * OD).astype(jnp.int32)
        current = lax.dynamic_slice_in_dim(accum_sigma, start_row, OD, 0)
        return lax.dynamic_update_slice_in_dim(accum_sigma, current + contribution, start_row, 0)

    def visit(accum_sigma, flat_index):
        domain = flat_index // PMAX
        position = flat_index % PMAX
        occ_first = pair_list[domain, position, 0]
        occ_second = pair_list[domain, position, 1]
        partner = occ_second // OD
        row_first = occ_first - domain * OD
        row_second = ((partner - domain) % NDOM) * OD + occ_second % OD

        def pair_step(running):
            b_first = slab_table[domain, row_first]
            b_second = slab_table[domain, row_second]
            c_first = coupling_table[domain, row_first]
            c_second = coupling_table[domain, row_second]
            z_first = dressed(c_first, domain)
            z_second = dressed(c_second, partner)
            coupled = product("kqa,qb->kab", z_first, b_second) + product("qa,kqb->kab", b_first, z_second)
            denominator = levels(domain)[None, :, None] + levels(partner)[None, None, :] - occ_energy[occ_first] - occ_energy[occ_second] - root_shift[:, None, None]
            doubles = (coupled / denominator).astype(jnp.bfloat16)
            gamma_first = product("kab,qb->kqa", doubles, b_second).astype(jnp.bfloat16)
            gamma_second = product("kab,qa->kqb", doubles, b_first).astype(jnp.bfloat16)
            sigma_first = -product("lq,kqa->lka", c_first, gamma_first)
            sigma_second = -product("lq,kqb->lkb", c_second, gamma_second)
            running = deposit(running, sigma_first, domain)
            return deposit(running, sigma_second, partner)

        accum_sigma = lax.cond(pair_count[domain] > position, pair_step, lambda unchanged: unchanged, accum_sigma)
        return accum_sigma, None

    initial = jnp.zeros((OCC, K, DV), jnp.float32)
    accum_sigma, _ = lax.scan(visit, initial, jnp.arange(NDOM * PMAX, dtype=jnp.int32))
    return accum_sigma
```

```python
import functools

import jax
import jax.numpy as jnp
from jax import lax
from jax.experimental import pallas as pl
from jax.experimental.pallas import tpu as pltpu
from jax.sharding import PartitionSpec as P

F32 = jnp.float32
BF16 = jnp.bfloat16
LANES = 128


def group_sums(parts):
    rows = parts[0].shape[0]
    index = lax.broadcasted_iota(jnp.int32, parts[0].shape, 0)
    step = 1
    while len(parts) > 1:
        low = (index // step) % 2 == 0
        parts = [
            jnp.where(low, even, pltpu.roll(odd, step, 0)) + jnp.where(low, pltpu.roll(even, rows - step, 0), odd)
            for even, odd in zip(parts[::2], parts[1::2])
        ]
        step *= 2
    return parts[0]


def sigma_kernel(
    ndomain, span, slot_count, occ_domain, root_count,
    ints_hbm, couple_hbm, trial_hbm, level_hbm, occ_hbm, shift_hbm, count_hbm, blocks_hbm, pairs_hbm,
    out_ref,
    ints, couple, trial, level_table, occ_energy, root_shift, pair_count, vir_blocks, pairs,
    levels_col, trial_f32, mixed, recip, stage, landed,
    ints_sem, small_sem, send_sem, recv_sem,
):
    me = lax.axis_index("aux")
    slab_rows, fitting, virt = ints.shape
    width_blocks = virt // LANES
    rows = occ_domain * root_count
    terms = 2 * occ_domain

    def ahead(steps):
        return lax.rem(me + steps, ndomain)

    scalars = [
        pltpu.make_async_copy(src, dst, small_sem.at[at])
        for at, (src, dst) in enumerate(
            [
                (level_hbm, level_table), (blocks_hbm, vir_blocks), (pairs_hbm, pairs), (occ_hbm, occ_energy),
                (shift_hbm, root_shift), (count_hbm, pair_count), (couple_hbm, couple),
            ]
        )
    ]
    for copy in scalars:
        copy.start()
    trial_sem = small_sem.at[len(scalars)]
    for steps in range(span):
        pltpu.make_async_copy(
            trial_hbm.at[pl.ds(ahead(steps) * occ_domain, occ_domain)],
            trial.at[pl.ds(steps * occ_domain, occ_domain)],
            trial_sem,
        ).start()
    big = pltpu.make_async_copy(ints_hbm, ints, ints_sem)
    big.start()

    barrier = pltpu.get_barrier_semaphore()
    for steps in range(1, span):
        for other in (ahead(steps), ahead(ndomain - steps)):
            pl.semaphore_signal(
                barrier, inc=1, device_id={"aux": other}, device_id_type=pl.DeviceIdType.MESH
            )

    for copy in scalars:
        copy.wait()
    pltpu.make_async_copy(trial_hbm.at[pl.ds(0, span * occ_domain)], trial, trial_sem).wait()

    def level_rows(relative):
        return [level_table[pl.ds(vir_blocks[block, ahead(relative)], 1), :] for block in range(width_blocks)]

    for block, row in enumerate(level_rows(0)):
        levels_col[pl.ds(block * LANES, LANES), :] = jnp.broadcast_to(row, (LANES, LANES)).T

    slots = []
    for slot in range(slot_count):
        occ_first = pairs[slot, 0, me]
        occ_second = pairs[slot, 1, me]
        relative = lax.rem(occ_second // occ_domain - me + ndomain, ndomain)
        relative = jnp.maximum(jnp.minimum(relative, span - 1), 1)
        first = lax.rem(occ_first, occ_domain)
        second = relative * occ_domain + lax.rem(occ_second, occ_domain)
        slots.append((relative, first, second, occ_energy[occ_first] + occ_energy[occ_second]))

    col = jnp.concatenate([levels_col[...]] * width_blocks, axis=1)
    for slot, (relative, first, second, energy) in enumerate(slots):
        level_row = jnp.concatenate(level_rows(relative), axis=1) - energy
        for root in range(0, root_count, 2):
            dens = [col + (level_row - root_shift[at]) for at in range(root, min(root + 2, root_count))]
            if len(dens) == 2:
                both = 1.0 / (dens[0] * dens[1])
                values = [both * dens[1], both * dens[0]]
            else:
                values = [1.0 / dens[0]]
            for at, value in enumerate(values):
                recip[slot, :, pl.ds((root + at) * virt, virt)] = value.astype(BF16)

    for relative in range(span):
        for own in range(occ_domain):
            trial_f32[relative, pl.ds(own * root_count, root_count), :] = trial[relative * occ_domain + own].astype(F32)
    couple_all = jnp.concatenate([couple[row].astype(F32) for row in range(slab_rows)], axis=0).astype(BF16)

    big.wait()
    for row in range(0, slab_rows, 2):
        pair = jnp.concatenate([ints[row], ints[row + 1]], axis=1)
        both = jnp.dot(couple_all, pair, preferred_element_type=F32)
        mixed[row] = both[:, :virt]
        mixed[row + 1] = both[:, virt:]

    index = lax.broadcasted_iota(jnp.int32, (rows, virt), 0)
    low_bit = index % occ_domain == 0
    own_side = (index // occ_domain) % 2 == 0
    high_bit = index // terms == 0

    def pick(mask, values):
        return jnp.where(mask, jnp.broadcast_to(values[0], (rows, virt)), jnp.broadcast_to(values[1], (rows, virt)))

    def trial_terms(relative, root):
        return pick(
            low_bit, [trial_f32[relative, pl.ds(own * root_count + root, 1), :] for own in range(occ_domain)]
        )

    own_terms = [trial_terms(0, root) for root in range(root_count)]
    live_slots = pair_count[me]
    totals = [jnp.zeros((rows, virt), F32) for _ in range(span)]
    kept = []
    for slot, (relative, first, second, energy) in enumerate(slots):
        live = live_slots > slot
        mix_first = [mixed[first, pl.ds(second * occ_domain + own, 1), :] for own in range(occ_domain)]
        mix_second = [mixed[second, pl.ds(first * occ_domain + own, 1), :] for own in range(occ_domain)]
        first_terms = pick(low_bit, mix_first)
        second_terms = pick(low_bit, mix_second)
        left = [jnp.where(own_side, own_terms[root], first_terms) for root in range(root_count)]
        right = [jnp.where(own_side, second_terms, trial_terms(relative, root)) for root in range(root_count)]
        first_by = pick(high_bit, mix_first)
        second_by = pick(high_bit, mix_second)
        weights = [(value * first_by).astype(F32) for value in left]
        parts = []
        for root in range(0, root_count, 2):
            both = jnp.dot(
                jnp.concatenate(weights[root : root + 2], axis=0).astype(BF16),
                recip[slot, :, pl.ds(root * virt, 2 * virt)],
                preferred_element_type=F32,
            )
            parts.append(both[:rows, :virt] * right[root])
            parts.append(both[rows:, virt:] * right[root + 1])
        added = group_sums(parts)
        for steps in range(1, span):
            totals[steps] += jnp.where(jnp.logical_and(live, relative == steps), added, 0.0)
        kept.append((left, [value * second_by for value in right], live))

    for steps in range(1, span):
        stage[steps - 1] = totals[steps]
    pl.semaphore_wait(barrier, 2 * (span - 1))
    copies = []
    for steps in range(1, span):
        copy = pltpu.make_async_remote_copy(
            src_ref=stage.at[steps - 1],
            dst_ref=landed.at[steps - 1],
            send_sem=send_sem.at[steps - 1],
            recv_sem=recv_sem.at[steps - 1],
            device_id={"aux": ahead(steps)},
            device_id_type=pl.DeviceIdType.MESH,
        )
        copy.start()
        copies.append(copy)

    result = totals[0]
    nothing = jnp.zeros((rows, virt), F32)
    for slot, (left, weights, live) in enumerate(kept):
        parts = []
        for root in range(0, root_count, 2):
            block = jnp.concatenate(
                [
                    jnp.concatenate([weights[root], nothing], axis=1),
                    jnp.concatenate([nothing, weights[root + 1]], axis=1),
                ],
                axis=0,
            ).astype(BF16)
            both = lax.dot_general(
                block,
                recip[slot, :, pl.ds(root * virt, 2 * virt)],
                (((1,), (1,)), ((), ())),
                preferred_element_type=F32,
            )
            parts.append(both[:rows] * left[root])
            parts.append(both[rows:] * left[root + 1])
        result += jnp.where(live, group_sums(parts), 0.0)
    for copy in copies:
        copy.wait()
    for steps in range(1, span):
        result = result + landed[steps - 1]
    for own in range(occ_domain):
        out_ref[own] = result[own * root_count : (own + 1) * root_count]


def per_device(
    ints_ov, ints_oo, trial, occ_energy, vir_energy, root_shift, vir_blocks, pair_list, pair_count
):
    slab_rows, fitting, virt = ints_ov.shape
    occ_domain = ints_oo.shape[1]
    root_count = trial.shape[1]
    slot_count = pair_list.shape[1]
    span = slab_rows // occ_domain
    rows = occ_domain * root_count
    level_table = vir_energy.reshape(-1, LANES)
    blocks = vir_blocks.T
    pairs = pair_list.transpose(1, 2, 0)
    anywhere = pl.BlockSpec(memory_space=pl.ANY)
    return pl.pallas_call(
        functools.partial(
            sigma_kernel, lax.axis_size("aux"), span, slot_count, occ_domain, root_count
        ),
        out_shape=jax.ShapeDtypeStruct((occ_domain, root_count, virt), F32),
        in_specs=[anywhere] * 9,
        out_specs=pl.BlockSpec(memory_space=pltpu.VMEM),
        scratch_shapes=[
            pltpu.VMEM(ints_ov.shape, BF16),
            pltpu.VMEM(ints_oo.shape, BF16),
            pltpu.VMEM((span * occ_domain, root_count, virt), BF16),
            pltpu.VMEM(level_table.shape, F32),
            pltpu.SMEM(occ_energy.shape, F32),
            pltpu.SMEM(root_shift.shape, F32),
            pltpu.SMEM(pair_count.shape, jnp.int32),
            pltpu.SMEM(blocks.shape, jnp.int32),
            pltpu.SMEM(pairs.shape, jnp.int32),
            pltpu.VMEM((virt, LANES), F32),
            pltpu.VMEM((span, rows, virt), F32),
            pltpu.VMEM((slab_rows, slab_rows * occ_domain, virt), F32),
            pltpu.VMEM((slot_count, virt, root_count * virt), BF16),
            pltpu.VMEM((span - 1, rows, virt), F32),
            pltpu.VMEM((span - 1, rows, virt), F32),
            pltpu.SemaphoreType.DMA,
            pltpu.SemaphoreType.DMA((8,)),
            pltpu.SemaphoreType.DMA((span - 1,)),
            pltpu.SemaphoreType.DMA((span - 1,)),
        ],
        compiler_params=pltpu.CompilerParams(collective_id=0, has_side_effects=True),
        name="sigma",
    )(ints_ov, ints_oo, trial, level_table, occ_energy, root_shift, pair_count, blocks, pairs)


def solution(mesh):
    in_specs = (
        P(("job", "aux"), None, None),
        P(("job", "aux"), None, None),
        P("job", None, None),
        P("job"),
        P("job"),
        P("job"),
        P("job", None),
        P("job", None, None),
        P("job"),
    )
    out_specs = P(("job", "aux"), None, None)
    return jax.shard_map(
        per_device, mesh=mesh, in_specs=in_specs, out_specs=out_specs, check_vma=False
    )
```

```python
import functools

import jax
import jax.numpy as jnp
from jax import lax
from jax.experimental import pallas as pl
from jax.experimental.pallas import tpu as pltpu
from jax.sharding import PartitionSpec as P

F32 = jnp.float32
BF16 = jnp.bfloat16
LANES = 128
RECIP_STEP = 6
LOOPED = 4
CHUNK = 8
PAIRED = 3


def group_sums(parts):
    rows = parts[0].shape[0]
    index = lax.broadcasted_iota(jnp.int32, parts[0].shape, 0)
    step = 1
    while len(parts) > 1:
        low = (index // step) % 2 == 0
        parts = [
            jnp.where(low, even, pltpu.roll(odd, step, 0)) + jnp.where(low, pltpu.roll(even, rows - step, 0), odd)
            for even, odd in zip(parts[::2], parts[1::2])
        ]
        step *= 2
    return parts[0]


def sigma_kernel(
    ndomain, span, slot_count, occ_domain, root_count,
    ints_hbm, couple_hbm, trial_hbm, level_hbm, occ_hbm, shift_hbm, count_hbm, blocks_hbm, pairs_hbm,
    out_ref,
    ints, couple, trial, level_table, occ_energy, root_shift, pair_count, vir_blocks, pairs,
    levels_col, level_row_table, trial_f32, mixed, recip, stage, landed,
    ints_sem, small_sem, send_sem, recv_sem,
):
    me = lax.axis_index("aux")
    slab_rows, fitting, virt = ints.shape
    width_blocks = virt // LANES
    rows = occ_domain * root_count
    terms = 2 * occ_domain

    def ahead(steps):
        return lax.rem(me + steps, ndomain)

    scalars = [
        pltpu.make_async_copy(src, dst, small_sem.at[at])
        for at, (src, dst) in enumerate(
            [
                (level_hbm, level_table), (blocks_hbm, vir_blocks), (pairs_hbm, pairs), (occ_hbm, occ_energy),
                (shift_hbm, root_shift), (count_hbm, pair_count), (couple_hbm, couple),
            ]
        )
    ]
    for copy in scalars:
        copy.start()
    trial_sem = small_sem.at[len(scalars)]
    for steps in range(span):
        pltpu.make_async_copy(
            trial_hbm.at[pl.ds(ahead(steps) * occ_domain, occ_domain)],
            trial.at[pl.ds(steps * occ_domain, occ_domain)],
            trial_sem,
        ).start()
    big = [
        pltpu.make_async_copy(ints_hbm.at[pl.ds(at, CHUNK)], ints.at[pl.ds(at, CHUNK)], ints_sem.at[at // CHUNK])
        for at in range(0, slab_rows, CHUNK)
    ]
    for copy in big:
        copy.start()

    barrier = pltpu.get_barrier_semaphore()
    for steps in range(1, span):
        for other in (ahead(steps), ahead(ndomain - steps)):
            pl.semaphore_signal(
                barrier, inc=1, device_id={"aux": other}, device_id_type=pl.DeviceIdType.MESH
            )

    for copy in scalars[:-1]:
        copy.wait()

    def level_rows(relative):
        return [level_table[pl.ds(vir_blocks[block, ahead(relative)], 1), :] for block in range(width_blocks)]

    for block, row in enumerate(level_rows(0)):
        levels_col[pl.ds(block * LANES, LANES), :] = jnp.broadcast_to(row, (LANES, LANES)).T

    slots = []
    for slot in range(slot_count):
        occ_first = pairs[slot, 0, me]
        occ_second = pairs[slot, 1, me]
        relative = lax.rem(occ_second // occ_domain - me + ndomain, ndomain)
        relative = jnp.maximum(jnp.minimum(relative, span - 1), 1)
        first = lax.rem(occ_first, occ_domain)
        second = relative * occ_domain + lax.rem(occ_second, occ_domain)
        slots.append((relative, first, second, occ_energy[occ_first] + occ_energy[occ_second]))

    for slot, (relative, first, second, energy) in enumerate(slots):
        level_row = jnp.concatenate(level_rows(relative), axis=1) - energy
        for root in range(root_count):
            level_row_table[pl.ds(slot * root_count + root, 1), :] = level_row - root_shift[root]

    def fill_recip(place, chosen):
        start = pl.multiple_of(place * 16, 16)
        col = levels_col[pl.ds(start, 16), :]
        for block in range(width_blocks):
            for slot in chosen:
                for root in range(0, root_count, 2):
                    dens = [
                        col + level_row_table[pl.ds(slot * root_count + at, 1), pl.ds(block * LANES, LANES)]
                        for at in range(root, root + 2)
                    ]
                    if slot % 4 >= PAIRED:
                        values = [1.0 / den for den in dens]
                    else:
                        both = 1.0 / (dens[0] * dens[1])
                        values = [both * dens[1], both * dens[0]]
                    for at, value in enumerate(values):
                        recip[slot, (root + at) * width_blocks + block, place] = value.astype(BF16)

    def recip_rows(step, carry):
        for piece in range(RECIP_STEP):
            fill_recip(step * RECIP_STEP + piece, range(LOOPED))
        return carry

    lax.fori_loop(0, virt // 16 // RECIP_STEP, recip_rows, 0)

    def recip_pair(slot, root):
        return jnp.concatenate(
            [recip[slot, root * width_blocks + at].reshape(virt, LANES) for at in range(2 * width_blocks)], axis=1
        )

    scalars[-1].wait()
    pltpu.make_async_copy(trial_hbm.at[pl.ds(0, span * occ_domain)], trial, trial_sem).wait()
    for relative in range(span):
        for own in range(occ_domain):
            trial_f32[relative, pl.ds(own * root_count, root_count), :] = trial[relative * occ_domain + own].astype(F32)
    couple_all = jnp.concatenate([couple[row].astype(F32) for row in range(slab_rows)], axis=0).astype(BF16)

    for place in range(virt // 16):
        fill_recip(place, range(LOOPED, slot_count))
    for row in range(0, slab_rows, 2):
        if row % CHUNK == 0:
            big[row // CHUNK].wait()
        pair = jnp.concatenate([ints[row], ints[row + 1]], axis=1)
        both = jnp.dot(couple_all, pair, preferred_element_type=F32)
        mixed[row] = both[:, :virt]
        mixed[row + 1] = both[:, virt:]

    index = lax.broadcasted_iota(jnp.int32, (rows, virt), 0)
    low_bit = index % occ_domain == 0
    own_side = (index // occ_domain) % 2 == 0
    high_bit = index // terms == 0

    def pick(mask, values):
        return jnp.where(mask, jnp.broadcast_to(values[0], (rows, virt)), jnp.broadcast_to(values[1], (rows, virt)))

    def trial_terms(relative, root):
        return pick(
            low_bit, [trial_f32[relative, pl.ds(own * root_count + root, 1), :] for own in range(occ_domain)]
        )

    own_terms = [trial_terms(0, root) for root in range(root_count)]
    live_slots = pair_count[me]
    totals = [jnp.zeros((rows, virt), F32) for _ in range(span)]
    kept = []
    for slot, (relative, first, second, energy) in enumerate(slots):
        live = live_slots > slot
        mix_first = [mixed[first, pl.ds(second * occ_domain + own, 1), :] for own in range(occ_domain)]
        mix_second = [mixed[second, pl.ds(first * occ_domain + own, 1), :] for own in range(occ_domain)]
        first_terms = pick(low_bit, mix_first)
        second_terms = pick(low_bit, mix_second)
        left = [jnp.where(own_side, own_terms[root], first_terms) for root in range(root_count)]
        right = [jnp.where(own_side, second_terms, trial_terms(relative, root)) for root in range(root_count)]
        first_by = pick(high_bit, mix_first)
        second_by = pick(high_bit, mix_second)
        weights = [(value * first_by).astype(F32) for value in left]
        parts = []
        for root in range(0, root_count, 2):
            both = jnp.dot(
                jnp.concatenate(weights[root : root + 2], axis=0).astype(BF16),
                recip_pair(slot, root),
                preferred_element_type=F32,
            )
            parts.append(both[:rows, :virt] * right[root])
            parts.append(both[rows:, virt:] * right[root + 1])
        added = group_sums(parts)
        for steps in range(1, span):
            totals[steps] += jnp.where(jnp.logical_and(live, relative == steps), added, 0.0)
        kept.append((left, [value * second_by for value in right], live))

    for steps in range(1, span):
        stage[steps - 1] = totals[steps]
    pl.semaphore_wait(barrier, 2 * (span - 1))
    copies = []
    for steps in range(1, span):
        copy = pltpu.make_async_remote_copy(
            src_ref=stage.at[steps - 1],
            dst_ref=landed.at[steps - 1],
            send_sem=send_sem.at[steps - 1],
            recv_sem=recv_sem.at[steps - 1],
            device_id={"aux": ahead(steps)},
            device_id_type=pl.DeviceIdType.MESH,
        )
        copy.start()
        copies.append(copy)

    result = totals[0]
    nothing = jnp.zeros((rows, virt), F32)
    for slot, (left, weights, live) in enumerate(kept):
        parts = []
        for root in range(0, root_count, 2):
            block = jnp.concatenate(
                [
                    jnp.concatenate([weights[root], nothing], axis=1),
                    jnp.concatenate([nothing, weights[root + 1]], axis=1),
                ],
                axis=0,
            ).astype(BF16)
            both = lax.dot_general(
                block,
                recip_pair(slot, root),
                (((1,), (1,)), ((), ())),
                preferred_element_type=F32,
            )
            parts.append(both[:rows] * left[root])
            parts.append(both[rows:] * left[root + 1])
        result += jnp.where(live, group_sums(parts), 0.0)
    for copy in copies:
        copy.wait()
    for steps in range(1, span):
        result = result + landed[steps - 1]
    for own in range(occ_domain):
        out_ref[own] = result[own * root_count : (own + 1) * root_count]


def per_device(
    ints_ov, ints_oo, trial, occ_energy, vir_energy, root_shift, vir_blocks, pair_list, pair_count
):
    slab_rows, fitting, virt = ints_ov.shape
    occ_domain = ints_oo.shape[1]
    root_count = trial.shape[1]
    slot_count = pair_list.shape[1]
    span = slab_rows // occ_domain
    rows = occ_domain * root_count
    level_table = vir_energy.reshape(-1, LANES)
    blocks = vir_blocks.T
    pairs = pair_list.transpose(1, 2, 0)
    anywhere = pl.BlockSpec(memory_space=pl.ANY)
    return pl.pallas_call(
        functools.partial(
            sigma_kernel, lax.axis_size("aux"), span, slot_count, occ_domain, root_count
        ),
        out_shape=pltpu.VMEM((occ_domain, root_count, virt), F32),
        in_specs=[anywhere] * 9,
        out_specs=pl.BlockSpec(memory_space=pltpu.VMEM),
        scratch_shapes=[
            pltpu.VMEM(ints_ov.shape, BF16),
            pltpu.VMEM(ints_oo.shape, BF16),
            pltpu.VMEM((span * occ_domain, root_count, virt), BF16),
            pltpu.VMEM(level_table.shape, F32),
            pltpu.SMEM(occ_energy.shape, F32),
            pltpu.SMEM(root_shift.shape, F32),
            pltpu.SMEM(pair_count.shape, jnp.int32),
            pltpu.SMEM(blocks.shape, jnp.int32),
            pltpu.SMEM(pairs.shape, jnp.int32),
            pltpu.VMEM((virt, LANES), F32),
            pltpu.VMEM((slot_count * root_count, virt), F32),
            pltpu.VMEM((span, rows, virt), F32),
            pltpu.VMEM((slab_rows, slab_rows * occ_domain, virt), F32),
            pltpu.VMEM((slot_count, root_count * virt // LANES, virt // 16, 16, LANES), BF16),
            pltpu.VMEM((span - 1, rows, virt), F32),
            pltpu.VMEM((span - 1, rows, virt), F32),
            pltpu.SemaphoreType.DMA((slab_rows // CHUNK,)),
            pltpu.SemaphoreType.DMA((8,)),
            pltpu.SemaphoreType.DMA((span - 1,)),
            pltpu.SemaphoreType.DMA((span - 1,)),
        ],
        compiler_params=pltpu.CompilerParams(collective_id=0, has_side_effects=True),
        name="sigma",
    )(ints_ov, ints_oo, trial, level_table, occ_energy, root_shift, pair_count, blocks, pairs)


def solution(mesh):
    in_specs = (
        P(("job", "aux"), None, None),
        P(("job", "aux"), None, None),
        P("job", None, None),
        P("job"),
        P("job"),
        P("job"),
        P("job", None),
        P("job", None, None),
        P("job"),
    )
    out_specs = P(("job", "aux"), None, None)
    return jax.shard_map(
        per_device, mesh=mesh, in_specs=in_specs, out_specs=out_specs, check_vma=False
    )
```

```python
import functools

import jax
import jax.numpy as jnp
from jax import lax
from jax.experimental import pallas as pl
from jax.experimental.pallas import tpu as pltpu
from jax.sharding import PartitionSpec as P

F32 = jnp.float32
BF16 = jnp.bfloat16
LANES = 128
PAIRED = 2
SPREAD = 64
ORDER = (
    "R00", "R01", "Wo", "D00", "D01", "R10", "R11", "D10",
    "D11", "R20", "R21", "D20", "D21", "R30", "Wf", "Mf",
    "R31", "D30", "D31",
)


def group_sums(parts):
    rows = parts[0].shape[0]
    index = lax.broadcasted_iota(jnp.int32, parts[0].shape, 0)
    step = 1
    while len(parts) > 1:
        low = (index // step) % 2 == 0
        parts = [
            jnp.where(low, even, pltpu.roll(odd, step, 0)) + jnp.where(low, pltpu.roll(even, rows - step, 0), odd)
            for even, odd in zip(parts[::2], parts[1::2])
        ]
        step *= 2
    return parts[0]


def sigma_kernel(
    ndomain, span, slot_count, occ_domain, root_count,
    ints_hbm, couple_hbm, trial_hbm, level_hbm, occ_hbm, shift_hbm, count_hbm, blocks_hbm, pairs_hbm,
    out_ref,
    ints, couple, trial, level_table, occ_energy, root_shift, pair_count, vir_blocks, pairs,
    levels_col, level_row_table, spread_ref, trial_f32, mixed_own, mixed_far, couple_ref, product, recip, stage, landed,
    ints_sem, small_sem, send_sem, recv_sem,
):
    me = lax.axis_index("aux")
    slab_rows, fitting, virt = ints.shape
    width_blocks = virt // LANES
    rows = occ_domain * root_count
    terms = 2 * occ_domain
    far_rows = slab_rows - occ_domain

    def ahead(steps):
        return lax.rem(me + steps, ndomain)

    trial_sem = small_sem.at[7]
    for steps in range(span):
        pltpu.make_async_copy(
            trial_hbm.at[pl.ds(ahead(steps) * occ_domain, occ_domain)],
            trial.at[pl.ds(steps * occ_domain, occ_domain)],
            trial_sem,
        ).start()
    scalars = [
        pltpu.make_async_copy(src, dst, small_sem.at[at])
        for at, (src, dst) in enumerate(
            [
                (level_hbm, level_table), (blocks_hbm, vir_blocks), (pairs_hbm, pairs), (occ_hbm, occ_energy),
                (shift_hbm, root_shift), (count_hbm, pair_count), (couple_hbm, couple),
            ]
        )
    ]
    for copy in scalars:
        copy.start()
    own_copy = pltpu.make_async_copy(
        ints_hbm.at[pl.ds(0, occ_domain)], ints.at[pl.ds(0, occ_domain)], ints_sem.at[0]
    )
    far_copy = pltpu.make_async_copy(
        ints_hbm.at[pl.ds(occ_domain, far_rows)], ints.at[pl.ds(occ_domain, far_rows)], ints_sem.at[1]
    )
    own_copy.start()
    far_copy.start()

    barrier = pltpu.get_barrier_semaphore()
    for steps in range(1, span):
        for other in (ahead(steps), ahead(ndomain - steps)):
            pl.semaphore_signal(
                barrier, inc=1, device_id={"aux": other}, device_id_type=pl.DeviceIdType.MESH
            )

    def factors(shape, axis, count):
        at = lax.broadcasted_iota(jnp.int32, shape, axis) % count
        return jnp.exp2(at.astype(F32) * (1.0 / count))

    spread = factors((SPREAD, virt), 0, SPREAD) * factors((SPREAD, virt), 1, LANES)
    spread_ref[...] = spread
    row_scale = factors((rows, virt), 1, SPREAD)
    column_scale = factors((rows, virt), 1, LANES)

    for copy in scalars[:-1]:
        copy.wait()

    def level_rows(relative):
        return [level_table[pl.ds(vir_blocks[block, ahead(relative)], 1), :] for block in range(width_blocks)]

    tall = jnp.concatenate([spread_ref[:, :LANES]] * (LANES // SPREAD), axis=0)
    for block, row in enumerate(level_rows(0)):
        levels_col[pl.ds(block * LANES, LANES), :] = jnp.broadcast_to(row, (LANES, LANES)).T * tall

    slots = []
    for slot in range(slot_count):
        occ_first = pairs[slot, 0, me]
        occ_second = pairs[slot, 1, me]
        relative = lax.rem(occ_second // occ_domain - me + ndomain, ndomain)
        relative = jnp.maximum(jnp.minimum(relative, span - 1), 1)
        first = lax.rem(occ_first, occ_domain)
        second = relative * occ_domain + lax.rem(occ_second, occ_domain)
        slots.append((relative, first, second, occ_energy[occ_first] + occ_energy[occ_second]))

    def fill_levels(slot):
        relative, first, second, energy = slots[slot]
        level_row = jnp.concatenate(level_rows(relative), axis=1) - energy
        for root in range(root_count):
            level_row_table[slot * root_count + root] = (level_row - root_shift[root]) * spread_ref[...]

    places = virt // 16

    def fill_recip(slot, root, chosen):
        for place in chosen:
            col = levels_col[pl.ds(place * 16, 16), :]
            for block in range(width_blocks):
                dens = [
                    col
                    + level_row_table[
                        slot * root_count + at, pl.ds(place * 16 % SPREAD, 16), pl.ds(block * LANES, LANES)
                    ]
                    for at in (root, root + 1)
                ]
                if (place + block) % 4 < PAIRED:
                    both = 1.0 / (dens[0] * dens[1])
                    values = [both * dens[1], both * dens[0]]
                else:
                    values = [1.0 / den for den in dens]
                for at, value in enumerate(values):
                    recip[slot, (root + at) * width_blocks + block, place] = value.astype(BF16)

    def recip_pair(slot, root):
        return jnp.concatenate(
            [recip[slot, root * width_blocks + at].reshape(virt, LANES) for at in range(2 * width_blocks)], axis=1
        )

    def mix(rows_pair, target):
        pair = jnp.concatenate([ints[row] for row in rows_pair], axis=1)
        both = jnp.dot(couple_ref[...], pair, preferred_element_type=F32)
        target[0] = both[:, :virt]
        target[1] = both[:, virt:]

    index = lax.broadcasted_iota(jnp.int32, (rows, virt), 0)
    low_bit = index % occ_domain == 0
    own_side = (index // occ_domain) % 2 == 0
    high_bit = index // terms == 0

    def pick(mask, values):
        return jnp.where(mask, jnp.broadcast_to(values[0], (rows, virt)), jnp.broadcast_to(values[1], (rows, virt)))

    def trial_terms(relative, root):
        return pick(
            low_bit, [trial_f32[relative, pl.ds(own * root_count + root, 1), :] for own in range(occ_domain)]
        )

    own_terms, lefts = [], {}

    def ready_own():
        scalars[-1].wait()
        pltpu.make_async_copy(trial_hbm.at[pl.ds(0, span * occ_domain)], trial, trial_sem).wait()
        for relative in range(span):
            for own in range(occ_domain):
                trial_f32[relative, pl.ds(own * root_count, root_count), :] = trial[
                    relative * occ_domain + own
                ].astype(F32)
        couple_ref[...] = jnp.concatenate([couple[row].astype(F32) for row in range(slab_rows)], axis=0).astype(BF16)
        own_copy.wait()
        for row in range(0, occ_domain, 2):
            mix((row, row + 1), mixed_own.at[pl.ds(row, 2)])
        own_terms.extend(trial_terms(0, root) for root in range(root_count))

    def lefts_of(slot):
        relative, first, second, energy = slots[slot]
        mix_first = [mixed_own[first, pl.ds(second * occ_domain + own, 1), :] for own in range(occ_domain)]
        first_terms = pick(low_bit, mix_first)
        left = [jnp.where(own_side, own_terms[root], first_terms) for root in range(root_count)]
        lefts[slot] = left, pick(high_bit, mix_first) * row_scale

    def multiply(slot, root):
        if root == 0:
            lefts_of(slot)
        left, first_by = lefts[slot]
        both = jnp.dot(
            jnp.concatenate([left[at] * first_by for at in (root, root + 1)], axis=0).astype(BF16),
            recip_pair(slot, root),
            preferred_element_type=F32,
        )
        product[slot, root] = both[:rows, :virt]
        product[slot, root + 1] = both[rows:, virt:]

    for step in ORDER:
        kind, at = step[0], step[1:]
        if kind == "R":
            slot, root = int(at[0]), 2 * int(at[1])
            if root == 0 and at[2:] != "b":
                fill_levels(slot)
            half = places * 2 // 3
            fill_recip(slot, root, {"": range(places), "a": range(half), "b": range(half, places)}[at[2:]])
        elif step == "Wo":
            ready_own()
        elif step == "Wf":
            far_copy.wait()
        elif step == "Mf":
            for slot in range(0, slot_count, 2):
                mix((slots[slot][2], slots[slot + 1][2]), mixed_far.at[pl.ds(slot, 2)])
        elif kind == "D":
            multiply(int(at[0]), 2 * int(at[1]))

    live_slots = pair_count[me]
    totals = [jnp.zeros((rows, virt), F32) for _ in range(span)]
    kept = []
    for slot, (relative, first, second, energy) in enumerate(slots):
        live = live_slots > slot
        mix_second = [
            mixed_far[slot, pl.ds(first * occ_domain + own, 1), :] for own in range(occ_domain)
        ]
        second_terms = pick(low_bit, mix_second)
        second_by = pick(high_bit, mix_second) * column_scale
        right = [jnp.where(own_side, second_terms, trial_terms(relative, root)) for root in range(root_count)]
        added = group_sums([product[slot, root] * right[root] for root in range(root_count)])
        for steps in range(1, span):
            totals[steps] += jnp.where(jnp.logical_and(live, relative == steps), added, 0.0)
        kept.append((lefts[slot][0], [value * second_by for value in right], live))

    for steps in range(1, span):
        stage[steps - 1] = totals[steps] * column_scale
    pl.semaphore_wait(barrier, 2 * (span - 1))
    copies = []
    for steps in range(1, span):
        copy = pltpu.make_async_remote_copy(
            src_ref=stage.at[steps - 1],
            dst_ref=landed.at[steps - 1],
            send_sem=send_sem.at[steps - 1],
            recv_sem=recv_sem.at[steps - 1],
            device_id={"aux": ahead(steps)},
            device_id_type=pl.DeviceIdType.MESH,
        )
        copy.start()
        copies.append(copy)

    result = totals[0]
    nothing = jnp.zeros((rows, virt), F32)
    for slot, (left, weights, live) in enumerate(kept):
        parts = []
        for root in range(0, root_count, 2):
            block = jnp.concatenate(
                [
                    jnp.concatenate([weights[root], nothing], axis=1),
                    jnp.concatenate([nothing, weights[root + 1]], axis=1),
                ],
                axis=0,
            ).astype(BF16)
            both = lax.dot_general(
                block,
                recip_pair(slot, root),
                (((1,), (1,)), ((), ())),
                preferred_element_type=F32,
            )
            parts.append(both[:rows] * left[root])
            parts.append(both[rows:] * left[root + 1])
        result += jnp.where(live, group_sums(parts), 0.0)
    result = result * row_scale
    for copy in copies:
        copy.wait()
    for steps in range(1, span):
        result = result + landed[steps - 1]
    for own in range(occ_domain):
        out_ref[own] = result[own * root_count : (own + 1) * root_count]


def per_device(
    ints_ov, ints_oo, trial, occ_energy, vir_energy, root_shift, vir_blocks, pair_list, pair_count
):
    slab_rows, fitting, virt = ints_ov.shape
    occ_domain = ints_oo.shape[1]
    root_count = trial.shape[1]
    slot_count = pair_list.shape[1]
    span = slab_rows // occ_domain
    rows = occ_domain * root_count
    level_table = vir_energy.reshape(-1, LANES)
    blocks = vir_blocks.T
    pairs = pair_list.transpose(1, 2, 0)
    anywhere = pl.BlockSpec(memory_space=pl.ANY)
    return pl.pallas_call(
        functools.partial(
            sigma_kernel, lax.axis_size("aux"), span, slot_count, occ_domain, root_count
        ),
        out_shape=pltpu.VMEM((occ_domain, root_count, virt), F32),
        in_specs=[anywhere] * 9,
        out_specs=pl.BlockSpec(memory_space=pltpu.VMEM),
        scratch_shapes=[
            pltpu.VMEM(ints_ov.shape, BF16),
            pltpu.VMEM(ints_oo.shape, BF16),
            pltpu.VMEM((span * occ_domain, root_count, virt), BF16),
            pltpu.VMEM(level_table.shape, F32),
            pltpu.SMEM(occ_energy.shape, F32),
            pltpu.SMEM(root_shift.shape, F32),
            pltpu.SMEM(pair_count.shape, jnp.int32),
            pltpu.SMEM(blocks.shape, jnp.int32),
            pltpu.SMEM(pairs.shape, jnp.int32),
            pltpu.VMEM((virt, LANES), F32),
            pltpu.VMEM((slot_count * root_count, SPREAD, virt), F32),
            pltpu.VMEM((SPREAD, virt), F32),
            pltpu.VMEM((span, rows, virt), F32),
            pltpu.VMEM((occ_domain, slab_rows * occ_domain, virt), F32),
            pltpu.VMEM((slot_count, slab_rows * occ_domain, virt), F32),
            pltpu.VMEM((slab_rows * occ_domain, fitting), BF16),
            pltpu.VMEM((slot_count, root_count, rows, virt), F32),
            pltpu.VMEM((slot_count, root_count * virt // LANES, virt // 16, 16, LANES), BF16),
            pltpu.VMEM((span - 1, rows, virt), F32),
            pltpu.VMEM((span - 1, rows, virt), F32),
            pltpu.SemaphoreType.DMA((2,)),
            pltpu.SemaphoreType.DMA((8,)),
            pltpu.SemaphoreType.DMA((span - 1,)),
            pltpu.SemaphoreType.DMA((span - 1,)),
        ],
        compiler_params=pltpu.CompilerParams(collective_id=0, has_side_effects=True),
        name="sigma",
    )(ints_ov, ints_oo, trial, level_table, occ_energy, root_shift, pair_count, blocks, pairs)


def solution(mesh):
    in_specs = (
        P(("job", "aux"), None, None),
        P(("job", "aux"), None, None),
        P("job", None, None),
        P("job"),
        P("job"),
        P("job"),
        P("job", None),
        P("job", None, None),
        P("job"),
    )
    out_specs = P(("job", "aux"), None, None)
    return jax.shard_map(
        per_device, mesh=mesh, in_specs=in_specs, out_specs=out_specs, check_vma=False
    )
```

```python
import functools

import jax
import jax.numpy as jnp
from jax import lax
from jax.experimental import pallas as pl
from jax.experimental.pallas import tpu as pltpu
from jax.sharding import PartitionSpec as P

F32 = jnp.float32
BF16 = jnp.bfloat16
LANES = 128
PAIRED = 2
SPREAD = 64
ORDER = (
    "R00", "Wo", "R01", "D00", "D01", "R10", "R11", "D10",
    "D11", "R20", "R21", "D20", "D21", "R30", "Wf", "Mf",
    "R31", "D30", "D31",
)


def group_sums(parts):
    rows = parts[0].shape[0]
    index = lax.broadcasted_iota(jnp.int32, parts[0].shape, 0)
    step = 1
    while len(parts) > 1:
        low = (index // step) % 2 == 0
        parts = [
            jnp.where(low, even, pltpu.roll(odd, step, 0)) + jnp.where(low, pltpu.roll(even, rows - step, 0), odd)
            for even, odd in zip(parts[::2], parts[1::2])
        ]
        step *= 2
    return parts[0]


def sigma_kernel(
    ndomain, span, slot_count, occ_domain, root_count,
    ints_hbm, couple_hbm, trial_hbm, level_hbm, occ_hbm, shift_hbm, count_hbm, blocks_hbm, pairs_hbm,
    out_ref,
    ints, couple, trial, level_table, occ_energy, root_shift, pair_count, vir_blocks, pairs,
    levels_col, level_row_table, spread_ref, trial_f32, mixed_own, mixed_far, couple_ref, product, recip, stage, landed,
    ints_sem, small_sem, send_sem, recv_sem,
):
    me = lax.axis_index("aux")
    slab_rows, fitting, virt = ints.shape
    width_blocks = virt // LANES
    rows = occ_domain * root_count
    terms = 2 * occ_domain
    far_rows = slab_rows - occ_domain

    def ahead(steps):
        return lax.rem(me + steps, ndomain)

    trial_sem = small_sem.at[7]
    for steps in range(span):
        pltpu.make_async_copy(
            trial_hbm.at[pl.ds(ahead(steps) * occ_domain, occ_domain)],
            trial.at[pl.ds(steps * occ_domain, occ_domain)],
            trial_sem,
        ).start()
    scalars = [
        pltpu.make_async_copy(src, dst, small_sem.at[at])
        for at, (src, dst) in enumerate(
            [
                (level_hbm, level_table), (blocks_hbm, vir_blocks), (pairs_hbm, pairs), (occ_hbm, occ_energy),
                (shift_hbm, root_shift), (count_hbm, pair_count), (couple_hbm, couple),
            ]
        )
    ]
    for copy in scalars:
        copy.start()
    own_copy = pltpu.make_async_copy(
        ints_hbm.at[pl.ds(0, occ_domain)], ints.at[pl.ds(0, occ_domain)], ints_sem.at[0]
    )
    far_copy = pltpu.make_async_copy(
        ints_hbm.at[pl.ds(occ_domain, far_rows)], ints.at[pl.ds(occ_domain, far_rows)], ints_sem.at[1]
    )
    own_copy.start()
    far_copy.start()

    barrier = pltpu.get_barrier_semaphore()
    for steps in range(1, span):
        for other in (ahead(steps), ahead(ndomain - steps)):
            pl.semaphore_signal(
                barrier, inc=1, device_id={"aux": other}, device_id_type=pl.DeviceIdType.MESH
            )

    def factors(shape, axis, count):
        at = lax.broadcasted_iota(jnp.int32, shape, axis) % count
        return jnp.exp2(at.astype(F32) * (1.0 / count))

    spread = factors((SPREAD, virt), 0, SPREAD) * factors((SPREAD, virt), 1, LANES)
    spread_ref[...] = spread
    row_scale = factors((rows, virt), 1, SPREAD)
    column_scale = factors((rows, virt), 1, LANES)

    for copy in scalars[:-1]:
        copy.wait()

    def level_rows(relative):
        return [level_table[pl.ds(vir_blocks[block, ahead(relative)], 1), :] for block in range(width_blocks)]

    tall = jnp.concatenate([spread_ref[:, :LANES]] * (LANES // SPREAD), axis=0)
    for block, row in enumerate(level_rows(0)):
        levels_col[pl.ds(block * LANES, LANES), :] = jnp.broadcast_to(row, (LANES, LANES)).T * tall

    slots = []
    for slot in range(slot_count):
        occ_first = pairs[slot, 0, me]
        occ_second = pairs[slot, 1, me]
        relative = lax.rem(occ_second // occ_domain - me + ndomain, ndomain)
        relative = jnp.maximum(jnp.minimum(relative, span - 1), 1)
        first = lax.rem(occ_first, occ_domain)
        second = relative * occ_domain + lax.rem(occ_second, occ_domain)
        slots.append((relative, first, second, occ_energy[occ_first] + occ_energy[occ_second]))

    def fill_levels(slot):
        relative, first, second, energy = slots[slot]
        level_row = jnp.concatenate(level_rows(relative), axis=1) - energy
        for root in range(root_count):
            level_row_table[slot * root_count + root] = (level_row - root_shift[root]) * spread_ref[...]

    places = virt // 16

    def fill_recip(slot, root, chosen):
        for block in range(width_blocks):
            for piece in range(0, SPREAD, 16):
                level = [
                    level_row_table[slot * root_count + at, pl.ds(piece, 16), pl.ds(block * LANES, LANES)]
                    for at in (root, root + 1)
                ]
                for place in chosen:
                    if place * 16 % SPREAD != piece:
                        continue
                    col = levels_col[pl.ds(place * 16, 16), :]
                    dens = [col + row for row in level]
                    if (place * 16 // SPREAD + block) % 4 < PAIRED:
                        both = 1.0 / (dens[0] * dens[1])
                        values = [both * dens[1], both * dens[0]]
                    else:
                        values = [1.0 / den for den in dens]
                    for at, value in enumerate(values):
                        recip[slot, (root + at) * width_blocks + block, place] = value.astype(BF16)

    def recip_pair(slot, root):
        return jnp.concatenate(
            [recip[slot, root * width_blocks + at].reshape(virt, LANES) for at in range(2 * width_blocks)], axis=1
        )

    def mix(rows_pair, target):
        pair = jnp.concatenate([ints[row] for row in rows_pair], axis=1)
        both = jnp.dot(couple_ref[...], pair, preferred_element_type=F32)
        target[0] = both[:, :virt]
        target[1] = both[:, virt:]

    index = lax.broadcasted_iota(jnp.int32, (rows, virt), 0)
    low_bit = index % occ_domain == 0
    own_side = (index // occ_domain) % 2 == 0
    high_bit = index // terms == 0

    def pick(mask, values):
        return jnp.where(mask, jnp.broadcast_to(values[0], (rows, virt)), jnp.broadcast_to(values[1], (rows, virt)))

    def trial_terms(relative, root):
        return pick(
            low_bit, [trial_f32[relative, pl.ds(own * root_count + root, 1), :] for own in range(occ_domain)]
        )

    own_terms, lefts = [], {}

    def ready_own():
        scalars[-1].wait()
        pltpu.make_async_copy(trial_hbm.at[pl.ds(0, span * occ_domain)], trial, trial_sem).wait()
        for relative in range(span):
            for own in range(occ_domain):
                trial_f32[relative, pl.ds(own * root_count, root_count), :] = trial[
                    relative * occ_domain + own
                ].astype(F32)
        couple_ref[...] = jnp.concatenate([couple[row].astype(F32) for row in range(slab_rows)], axis=0).astype(BF16)
        own_copy.wait()
        for row in range(0, occ_domain, 2):
            mix((row, row + 1), mixed_own.at[pl.ds(row, 2)])
        own_terms.extend(trial_terms(0, root) for root in range(root_count))

    def lefts_of(slot):
        relative, first, second, energy = slots[slot]
        mix_first = [mixed_own[first, pl.ds(second * occ_domain + own, 1), :] for own in range(occ_domain)]
        first_terms = pick(low_bit, mix_first)
        left = [jnp.where(own_side, own_terms[root], first_terms) for root in range(root_count)]
        lefts[slot] = left, pick(high_bit, mix_first) * row_scale

    def multiply(slot, root):
        if root == 0:
            lefts_of(slot)
        left, first_by = lefts[slot]
        both = jnp.dot(
            jnp.concatenate([left[at] * first_by for at in (root, root + 1)], axis=0).astype(BF16),
            recip_pair(slot, root),
            preferred_element_type=F32,
        )
        product[slot, root] = both[:rows, :virt]
        product[slot, root + 1] = both[rows:, virt:]

    for step in ORDER:
        kind, at = step[0], step[1:]
        if kind == "R":
            slot, root = int(at[0]), 2 * int(at[1])
            if root == 0 and at[2:] != "b":
                fill_levels(slot)
            half = places * 2 // 3
            fill_recip(slot, root, {"": range(places), "a": range(half), "b": range(half, places)}[at[2:]])
        elif step == "Wo":
            ready_own()
        elif step == "Wf":
            far_copy.wait()
        elif step == "Mf":
            for slot in range(0, slot_count, 2):
                mix((slots[slot][2], slots[slot + 1][2]), mixed_far.at[pl.ds(slot, 2)])
        elif kind == "D":
            multiply(int(at[0]), 2 * int(at[1]))

    live_slots = pair_count[me]
    totals = [jnp.zeros((rows, virt), F32) for _ in range(span)]
    kept = []
    for slot, (relative, first, second, energy) in enumerate(slots):
        live = live_slots > slot
        mix_second = [
            mixed_far[slot, pl.ds(first * occ_domain + own, 1), :] for own in range(occ_domain)
        ]
        second_terms = pick(low_bit, mix_second)
        second_by = pick(high_bit, mix_second) * column_scale
        right = [jnp.where(own_side, second_terms, trial_terms(relative, root)) for root in range(root_count)]
        added = group_sums([product[slot, root] * right[root] for root in range(root_count)])
        for steps in range(1, span):
            totals[steps] += jnp.where(jnp.logical_and(live, relative == steps), added, 0.0)
        kept.append((lefts[slot][0], [value * second_by for value in right], live))

    for steps in range(1, span):
        stage[steps - 1] = totals[steps] * column_scale
    pl.semaphore_wait(barrier, 2 * (span - 1))
    copies = []
    for steps in range(1, span):
        copy = pltpu.make_async_remote_copy(
            src_ref=stage.at[steps - 1],
            dst_ref=landed.at[steps - 1],
            send_sem=send_sem.at[steps - 1],
            recv_sem=recv_sem.at[steps - 1],
            device_id={"aux": ahead(steps)},
            device_id_type=pl.DeviceIdType.MESH,
        )
        copy.start()
        copies.append(copy)

    result = totals[0]
    nothing = jnp.zeros((rows, virt), F32)
    for slot, (left, weights, live) in enumerate(kept):
        parts = []
        for root in range(0, root_count, 2):
            block = jnp.concatenate(
                [
                    jnp.concatenate([weights[root], nothing], axis=1),
                    jnp.concatenate([nothing, weights[root + 1]], axis=1),
                ],
                axis=0,
            ).astype(BF16)
            both = lax.dot_general(
                block,
                recip_pair(slot, root),
                (((1,), (1,)), ((), ())),
                preferred_element_type=F32,
            )
            parts.append(both[:rows] * left[root])
            parts.append(both[rows:] * left[root + 1])
        result += jnp.where(live, group_sums(parts), 0.0)
    result = result * row_scale
    for copy in copies:
        copy.wait()
    for steps in range(1, span):
        result = result + landed[steps - 1]
    for own in range(occ_domain):
        out_ref[own] = result[own * root_count : (own + 1) * root_count]


def per_device(
    ints_ov, ints_oo, trial, occ_energy, vir_energy, root_shift, vir_blocks, pair_list, pair_count
):
    slab_rows, fitting, virt = ints_ov.shape
    occ_domain = ints_oo.shape[1]
    root_count = trial.shape[1]
    slot_count = pair_list.shape[1]
    span = slab_rows // occ_domain
    rows = occ_domain * root_count
    level_table = vir_energy.reshape(-1, LANES)
    blocks = vir_blocks.T
    pairs = pair_list.transpose(1, 2, 0)
    anywhere = pl.BlockSpec(memory_space=pl.ANY)
    return pl.pallas_call(
        functools.partial(
            sigma_kernel, lax.axis_size("aux"), span, slot_count, occ_domain, root_count
        ),
        out_shape=pltpu.VMEM((occ_domain, root_count, virt), F32),
        in_specs=[anywhere] * 9,
        out_specs=pl.BlockSpec(memory_space=pltpu.VMEM),
        scratch_shapes=[
            pltpu.VMEM(ints_ov.shape, BF16),
            pltpu.VMEM(ints_oo.shape, BF16),
            pltpu.VMEM((span * occ_domain, root_count, virt), BF16),
            pltpu.VMEM(level_table.shape, F32),
            pltpu.SMEM(occ_energy.shape, F32),
            pltpu.SMEM(root_shift.shape, F32),
            pltpu.SMEM(pair_count.shape, jnp.int32),
            pltpu.SMEM(blocks.shape, jnp.int32),
            pltpu.SMEM(pairs.shape, jnp.int32),
            pltpu.VMEM((virt, LANES), F32),
            pltpu.VMEM((slot_count * root_count, SPREAD, virt), F32),
            pltpu.VMEM((SPREAD, virt), F32),
            pltpu.VMEM((span, rows, virt), F32),
            pltpu.VMEM((occ_domain, slab_rows * occ_domain, virt), F32),
            pltpu.VMEM((slot_count, slab_rows * occ_domain, virt), F32),
            pltpu.VMEM((slab_rows * occ_domain, fitting), BF16),
            pltpu.VMEM((slot_count, root_count, rows, virt), F32),
            pltpu.VMEM((slot_count, root_count * virt // LANES, virt // 16, 16, LANES), BF16),
            pltpu.VMEM((span - 1, rows, virt), F32),
            pltpu.VMEM((span - 1, rows, virt), F32),
            pltpu.SemaphoreType.DMA((2,)),
            pltpu.SemaphoreType.DMA((8,)),
            pltpu.SemaphoreType.DMA((span - 1,)),
            pltpu.SemaphoreType.DMA((span - 1,)),
        ],
        compiler_params=pltpu.CompilerParams(collective_id=0, has_side_effects=True),
        name="sigma",
    )(ints_ov, ints_oo, trial, level_table, occ_energy, root_shift, pair_count, blocks, pairs)


def solution(mesh):
    in_specs = (
        P(("job", "aux"), None, None),
        P(("job", "aux"), None, None),
        P("job", None, None),
        P("job"),
        P("job"),
        P("job"),
        P("job", None),
        P("job", None, None),
        P("job"),
    )
    out_specs = P(("job", "aux"), None, None)
    return jax.shard_map(
        per_device, mesh=mesh, in_specs=in_specs, out_specs=out_specs, check_vma=False
    )
```

```python
import functools

import jax
import jax.numpy as jnp
from jax import lax
from jax.experimental import pallas as pl
from jax.experimental.pallas import tpu as pltpu
from jax.sharding import PartitionSpec as P

F32 = jnp.float32
BF16 = jnp.bfloat16
LANES = 128
PAIRED = 2
SPREAD = 64
ORDER = (
    "R00", "Wo", "R01", "D00", "D01", "R10", "R11", "D10",
    "D11", "R20", "R21", "D20", "D21", "R30", "Wf", "Mf",
    "R31", "D30", "D31",
)


def group_sums(parts):
    rows = parts[0].shape[0]
    index = lax.broadcasted_iota(jnp.int32, parts[0].shape, 0)
    step = 1
    while len(parts) > 1:
        low = (index // step) % 2 == 0
        parts = [
            jnp.where(low, even, pltpu.roll(odd, step, 0)) + jnp.where(low, pltpu.roll(even, rows - step, 0), odd)
            for even, odd in zip(parts[::2], parts[1::2])
        ]
        step *= 2
    return parts[0]


def sigma_kernel(
    ndomain, span, slot_count, occ_domain, root_count,
    ints_hbm, couple_hbm, trial_hbm, level_hbm, occ_hbm, shift_hbm, count_hbm, blocks_hbm, pairs_hbm,
    out_ref,
    ints, couple, trial, level_table, occ_energy, root_shift, pair_count, vir_blocks, pairs,
    levels_col, level_row_table, spread_ref, trial_f32, mixed_own, mixed_far, couple_ref, product, recip, stage, landed,
    ints_sem, small_sem, send_sem, recv_sem,
):
    me = lax.axis_index("aux")
    slab_rows, fitting, virt = ints.shape
    width_blocks = virt // LANES
    rows = occ_domain * root_count
    terms = 2 * occ_domain
    far_rows = slab_rows - occ_domain

    def ahead(steps):
        return lax.rem(me + steps, ndomain)

    scalars = [
        pltpu.make_async_copy(src, dst, small_sem.at[at])
        for at, (src, dst) in enumerate(
            [
                (level_hbm, level_table), (blocks_hbm, vir_blocks), (pairs_hbm, pairs), (occ_hbm, occ_energy),
                (shift_hbm, root_shift), (count_hbm, pair_count), (couple_hbm, couple),
            ]
        )
    ]
    for copy in scalars[:-1]:
        copy.start()
    own_copy = pltpu.make_async_copy(
        ints_hbm.at[pl.ds(0, occ_domain)], ints.at[pl.ds(0, occ_domain)], ints_sem.at[0]
    )
    far_copy = pltpu.make_async_copy(
        ints_hbm.at[pl.ds(occ_domain, far_rows)], ints.at[pl.ds(occ_domain, far_rows)], ints_sem.at[1]
    )
    own_copy.start()
    trial_sem = small_sem.at[7]
    for steps in range(span):
        pltpu.make_async_copy(
            trial_hbm.at[pl.ds(ahead(steps) * occ_domain, occ_domain)],
            trial.at[pl.ds(steps * occ_domain, occ_domain)],
            trial_sem,
        ).start()
    scalars[-1].start()
    far_copy.start()

    barrier = pltpu.get_barrier_semaphore()
    for steps in range(1, span):
        for other in (ahead(steps), ahead(ndomain - steps)):
            pl.semaphore_signal(
                barrier, inc=1, device_id={"aux": other}, device_id_type=pl.DeviceIdType.MESH
            )

    def factors(shape, axis, count):
        at = lax.broadcasted_iota(jnp.int32, shape, axis) % count
        return jnp.exp2(at.astype(F32) * (1.0 / count))

    spread = factors((SPREAD, virt), 0, SPREAD) * factors((SPREAD, virt), 1, LANES)
    spread_ref[...] = spread
    row_scale = factors((rows, virt), 1, SPREAD)
    column_scale = factors((rows, virt), 1, LANES)

    for copy in scalars[:-1]:
        copy.wait()

    def level_rows(relative):
        return [level_table[pl.ds(vir_blocks[block, ahead(relative)], 1), :] for block in range(width_blocks)]

    tall = jnp.concatenate([spread_ref[:, :LANES]] * (LANES // SPREAD), axis=0)
    for block, row in enumerate(level_rows(0)):
        levels_col[pl.ds(block * LANES, LANES), :] = jnp.broadcast_to(row, (LANES, LANES)).T * tall

    slots = []
    for slot in range(slot_count):
        occ_first = pairs[slot, 0, me]
        occ_second = pairs[slot, 1, me]
        relative = lax.rem(occ_second // occ_domain - me + ndomain, ndomain)
        relative = jnp.maximum(jnp.minimum(relative, span - 1), 1)
        first = lax.rem(occ_first, occ_domain)
        second = relative * occ_domain + lax.rem(occ_second, occ_domain)
        slots.append((relative, first, second, occ_energy[occ_first] + occ_energy[occ_second]))

    def fill_levels(slot):
        relative, first, second, energy = slots[slot]
        level_row = jnp.concatenate(level_rows(relative), axis=1) - energy
        for root in range(root_count):
            level_row_table[slot * root_count + root] = (level_row - root_shift[root]) * spread_ref[...]

    places = virt // 16

    def fill_recip(slot, root, chosen):
        for block in range(width_blocks):
            for piece in range(0, SPREAD, 16):
                level = [
                    level_row_table[slot * root_count + at, pl.ds(piece, 16), pl.ds(block * LANES, LANES)]
                    for at in (root, root + 1)
                ]
                for place in chosen:
                    if place * 16 % SPREAD != piece:
                        continue
                    col = levels_col[pl.ds(place * 16, 16), :]
                    dens = [col + row for row in level]
                    if (place * 16 // SPREAD + block) % 4 < PAIRED:
                        both = 1.0 / (dens[0] * dens[1])
                        values = [both * dens[1], both * dens[0]]
                    else:
                        values = [1.0 / den for den in dens]
                    for at, value in enumerate(values):
                        recip[slot, (root + at) * width_blocks + block, place] = value.astype(BF16)

    def recip_pair(slot, root):
        return jnp.concatenate(
            [recip[slot, root * width_blocks + at].reshape(virt, LANES) for at in range(2 * width_blocks)], axis=1
        )

    def mix(rows_pair, target):
        pair = jnp.concatenate([ints[row] for row in rows_pair], axis=1)
        both = jnp.dot(couple_ref[...], pair, preferred_element_type=F32)
        target[0] = both[:, :virt]
        target[1] = both[:, virt:]

    index = lax.broadcasted_iota(jnp.int32, (rows, virt), 0)
    low_bit = index % occ_domain == 0
    own_side = (index // occ_domain) % 2 == 0
    high_bit = index // terms == 0

    def pick(mask, values):
        return jnp.where(mask, jnp.broadcast_to(values[0], (rows, virt)), jnp.broadcast_to(values[1], (rows, virt)))

    def trial_terms(relative, root):
        return pick(
            low_bit, [trial_f32[relative, pl.ds(own * root_count + root, 1), :] for own in range(occ_domain)]
        )

    own_terms, lefts = [], {}

    def ready_own():
        scalars[-1].wait()
        pltpu.make_async_copy(trial_hbm.at[pl.ds(0, span * occ_domain)], trial, trial_sem).wait()
        for relative in range(span):
            for own in range(occ_domain):
                trial_f32[relative, pl.ds(own * root_count, root_count), :] = trial[
                    relative * occ_domain + own
                ].astype(F32)
        couple_ref[...] = jnp.concatenate([couple[row].astype(F32) for row in range(slab_rows)], axis=0).astype(BF16)
        own_copy.wait()
        for row in range(0, occ_domain, 2):
            mix((row, row + 1), mixed_own.at[pl.ds(row, 2)])
        own_terms.extend(trial_terms(0, root) for root in range(root_count))

    def lefts_of(slot):
        relative, first, second, energy = slots[slot]
        mix_first = [mixed_own[first, pl.ds(second * occ_domain + own, 1), :] for own in range(occ_domain)]
        first_terms = pick(low_bit, mix_first)
        left = [jnp.where(own_side, own_terms[root], first_terms) for root in range(root_count)]
        lefts[slot] = left, pick(high_bit, mix_first) * row_scale

    def multiply(slot, root):
        if root == 0:
            lefts_of(slot)
        left, first_by = lefts[slot]
        both = jnp.dot(
            jnp.concatenate([left[at] * first_by for at in (root, root + 1)], axis=0).astype(BF16),
            recip_pair(slot, root),
            preferred_element_type=F32,
        )
        product[slot, root] = both[:rows, :virt]
        product[slot, root + 1] = both[rows:, virt:]

    for step in ORDER:
        kind, at = step[0], step[1:]
        if kind == "R":
            slot, root = int(at[0]), 2 * int(at[1])
            if root == 0 and at[2:] != "b":
                fill_levels(slot)
            half = places * 2 // 3
            fill_recip(slot, root, {"": range(places), "a": range(half), "b": range(half, places)}[at[2:]])
        elif step == "Wo":
            ready_own()
        elif step == "Wf":
            far_copy.wait()
        elif step == "Mf":
            for slot in range(0, slot_count, 2):
                mix((slots[slot][2], slots[slot + 1][2]), mixed_far.at[pl.ds(slot, 2)])
        elif kind == "D":
            multiply(int(at[0]), 2 * int(at[1]))

    live_slots = pair_count[me]
    totals = [jnp.zeros((rows, virt), F32) for _ in range(span)]
    kept = []
    for slot, (relative, first, second, energy) in enumerate(slots):
        live = live_slots > slot
        mix_second = [
            mixed_far[slot, pl.ds(first * occ_domain + own, 1), :] for own in range(occ_domain)
        ]
        second_terms = pick(low_bit, mix_second)
        second_by = pick(high_bit, mix_second) * column_scale
        right = [jnp.where(own_side, second_terms, trial_terms(relative, root)) for root in range(root_count)]
        added = group_sums([product[slot, root] * right[root] for root in range(root_count)])
        for steps in range(1, span):
            totals[steps] += jnp.where(jnp.logical_and(live, relative == steps), added, 0.0)
        kept.append((lefts[slot][0], [value * second_by for value in right], live))

    for steps in range(1, span):
        stage[steps - 1] = totals[steps] * column_scale
    pl.semaphore_wait(barrier, 2 * (span - 1))
    copies = []
    for steps in range(1, span):
        copy = pltpu.make_async_remote_copy(
            src_ref=stage.at[steps - 1],
            dst_ref=landed.at[steps - 1],
            send_sem=send_sem.at[steps - 1],
            recv_sem=recv_sem.at[steps - 1],
            device_id={"aux": ahead(steps)},
            device_id_type=pl.DeviceIdType.MESH,
        )
        copy.start()
        copies.append(copy)

    result = totals[0]
    nothing = jnp.zeros((rows, virt), F32)
    for slot, (left, weights, live) in enumerate(kept):
        parts = []
        for root in range(0, root_count, 2):
            heads = [weights[at].astype(BF16).astype(F32) for at in (root, root + 1)]
            tails = [weights[at] - head for at, head in zip((root, root + 1), heads)]
            block = jnp.concatenate(
                [
                    jnp.concatenate([half[0], nothing] if at == 0 else [nothing, half[1]], axis=1)
                    for half in (heads, tails)
                    for at in (0, 1)
                ],
                axis=0,
            ).astype(BF16)
            both = lax.dot_general(
                block,
                recip_pair(slot, root),
                (((1,), (1,)), ((), ())),
                preferred_element_type=F32,
            )
            both = both[: 2 * rows] + both[2 * rows :]
            parts.append(both[:rows] * left[root])
            parts.append(both[rows:] * left[root + 1])
        result += jnp.where(live, group_sums(parts), 0.0)
    result = result * row_scale
    for copy in copies:
        copy.wait()
    for steps in range(1, span):
        result = result + landed[steps - 1]
    for own in range(occ_domain):
        out_ref[own] = result[own * root_count : (own + 1) * root_count]


def per_device(
    ints_ov, ints_oo, trial, occ_energy, vir_energy, root_shift, vir_blocks, pair_list, pair_count
):
    slab_rows, fitting, virt = ints_ov.shape
    occ_domain = ints_oo.shape[1]
    root_count = trial.shape[1]
    slot_count = pair_list.shape[1]
    span = slab_rows // occ_domain
    rows = occ_domain * root_count
    level_table = vir_energy.reshape(-1, LANES)
    blocks = vir_blocks.T
    pairs = pair_list.transpose(1, 2, 0)
    anywhere = pl.BlockSpec(memory_space=pl.ANY)
    return pl.pallas_call(
        functools.partial(
            sigma_kernel, lax.axis_size("aux"), span, slot_count, occ_domain, root_count
        ),
        out_shape=pltpu.VMEM((occ_domain, root_count, virt), F32),
        in_specs=[anywhere] * 9,
        out_specs=pl.BlockSpec(memory_space=pltpu.VMEM),
        scratch_shapes=[
            pltpu.VMEM(ints_ov.shape, BF16),
            pltpu.VMEM(ints_oo.shape, BF16),
            pltpu.VMEM((span * occ_domain, root_count, virt), BF16),
            pltpu.VMEM(level_table.shape, F32),
            pltpu.SMEM(occ_energy.shape, F32),
            pltpu.SMEM(root_shift.shape, F32),
            pltpu.SMEM(pair_count.shape, jnp.int32),
            pltpu.SMEM(blocks.shape, jnp.int32),
            pltpu.SMEM(pairs.shape, jnp.int32),
            pltpu.VMEM((virt, LANES), F32),
            pltpu.VMEM((slot_count * root_count, SPREAD, virt), F32),
            pltpu.VMEM((SPREAD, virt), F32),
            pltpu.VMEM((span, rows, virt), F32),
            pltpu.VMEM((occ_domain, slab_rows * occ_domain, virt), F32),
            pltpu.VMEM((slot_count, slab_rows * occ_domain, virt), F32),
            pltpu.VMEM((slab_rows * occ_domain, fitting), BF16),
            pltpu.VMEM((slot_count, root_count, rows, virt), F32),
            pltpu.VMEM((slot_count, root_count * virt // LANES, virt // 16, 16, LANES), BF16),
            pltpu.VMEM((span - 1, rows, virt), F32),
            pltpu.VMEM((span - 1, rows, virt), F32),
            pltpu.SemaphoreType.DMA((2,)),
            pltpu.SemaphoreType.DMA((8,)),
            pltpu.SemaphoreType.DMA((span - 1,)),
            pltpu.SemaphoreType.DMA((span - 1,)),
        ],
        compiler_params=pltpu.CompilerParams(collective_id=0, has_side_effects=True),
        name="sigma",
    )(ints_ov, ints_oo, trial, level_table, occ_energy, root_shift, pair_count, blocks, pairs)


def solution(mesh):
    in_specs = (
        P(("job", "aux"), None, None),
        P(("job", "aux"), None, None),
        P("job", None, None),
        P("job"),
        P("job"),
        P("job"),
        P("job", None),
        P("job", None, None),
        P("job"),
    )
    out_specs = P(("job", "aux"), None, None)
    return jax.shard_map(
        per_device, mesh=mesh, in_specs=in_specs, out_specs=out_specs, check_vma=False
    )
```

```python
import functools

import jax
import jax.numpy as jnp
from jax import lax
from jax.experimental import pallas as pl
from jax.experimental.pallas import tpu as pltpu
from jax.sharding import PartitionSpec as P

F32 = jnp.float32
BF16 = jnp.bfloat16
LANES = 128
PAIRED = 2
SPREAD = 32
ORDER = (
    "R00", "Wo", "R01", "D00", "D01", "R10", "R11", "D10",
    "D11", "R20", "R21", "D20", "D21", "R30", "Wf", "Mf",
    "R31", "D30", "D31",
)


def group_sums(parts):
    rows = parts[0].shape[0]
    index = lax.broadcasted_iota(jnp.int32, parts[0].shape, 0)
    step = 1
    while len(parts) > 1:
        low = (index // step) % 2 == 0
        parts = [
            jnp.where(low, even, pltpu.roll(odd, step, 0)) + jnp.where(low, pltpu.roll(even, rows - step, 0), odd)
            for even, odd in zip(parts[::2], parts[1::2])
        ]
        step *= 2
    return parts[0]


def sigma_kernel(
    ndomain, span, slot_count, occ_domain, root_count,
    ints_hbm, couple_hbm, trial_hbm, level_hbm, occ_hbm, shift_hbm, count_hbm, blocks_hbm, pairs_hbm,
    out_ref,
    ints, couple, trial, level_table, occ_energy, root_shift, pair_count, vir_blocks, pairs,
    levels_col, level_row_table, spread_ref, trial_f32, mixed_own, mixed_far, couple_ref, product, recip, stage, landed,
    ints_sem, small_sem, send_sem, recv_sem,
):
    me = lax.axis_index("aux")
    slab_rows, fitting, virt = ints.shape
    width_blocks = virt // LANES
    rows = occ_domain * root_count
    terms = 2 * occ_domain
    far_rows = slab_rows - occ_domain

    def ahead(steps):
        return lax.rem(me + steps, ndomain)

    scalars = [
        pltpu.make_async_copy(src, dst, small_sem.at[at])
        for at, (src, dst) in enumerate(
            [
                (level_hbm, level_table), (blocks_hbm, vir_blocks), (pairs_hbm, pairs), (occ_hbm, occ_energy),
                (shift_hbm, root_shift), (count_hbm, pair_count), (couple_hbm, couple),
            ]
        )
    ]
    for copy in scalars[:-1]:
        copy.start()
    own_copy = pltpu.make_async_copy(
        ints_hbm.at[pl.ds(0, occ_domain)], ints.at[pl.ds(0, occ_domain)], ints_sem.at[0]
    )
    far_copy = pltpu.make_async_copy(
        ints_hbm.at[pl.ds(occ_domain, far_rows)], ints.at[pl.ds(occ_domain, far_rows)], ints_sem.at[1]
    )
    own_copy.start()
    trial_sem = small_sem.at[7]
    for steps in range(span):
        pltpu.make_async_copy(
            trial_hbm.at[pl.ds(ahead(steps) * occ_domain, occ_domain)],
            trial.at[pl.ds(steps * occ_domain, occ_domain)],
            trial_sem,
        ).start()
    scalars[-1].start()
    far_copy.start()

    barrier = pltpu.get_barrier_semaphore()
    for steps in range(1, span):
        for other in (ahead(steps), ahead(ndomain - steps)):
            pl.semaphore_signal(
                barrier, inc=1, device_id={"aux": other}, device_id_type=pl.DeviceIdType.MESH
            )

    def factors(shape, axis, count):
        at = lax.broadcasted_iota(jnp.int32, shape, axis) % count
        return jnp.exp2(at.astype(F32) * (1.0 / count))

    spread = factors((SPREAD, virt), 0, SPREAD) * factors((SPREAD, virt), 1, LANES)
    spread_ref[...] = spread
    row_scale = factors((rows, virt), 1, SPREAD)
    column_scale = factors((rows, virt), 1, LANES)

    for copy in scalars[:-1]:
        copy.wait()

    def level_rows(relative):
        return [level_table[pl.ds(vir_blocks[block, ahead(relative)], 1), :] for block in range(width_blocks)]

    tall = jnp.concatenate([spread_ref[:, :LANES]] * (LANES // SPREAD), axis=0)
    for block, row in enumerate(level_rows(0)):
        levels_col[pl.ds(block * LANES, LANES), :] = jnp.broadcast_to(row, (LANES, LANES)).T * tall

    slots = []
    for slot in range(slot_count):
        occ_first = pairs[slot, 0, me]
        occ_second = pairs[slot, 1, me]
        relative = lax.rem(occ_second // occ_domain - me + ndomain, ndomain)
        relative = jnp.maximum(jnp.minimum(relative, span - 1), 1)
        first = lax.rem(occ_first, occ_domain)
        second = relative * occ_domain + lax.rem(occ_second, occ_domain)
        slots.append((relative, first, second, occ_energy[occ_first] + occ_energy[occ_second]))

    def fill_levels(slot):
        relative, first, second, energy = slots[slot]
        level_row = jnp.concatenate(level_rows(relative), axis=1) - energy
        for root in range(root_count):
            level_row_table[slot * root_count + root] = (level_row - root_shift[root]) * spread_ref[...]

    places = virt // 16

    def fill_recip(slot, root, chosen):
        for block in range(width_blocks):
            for piece in range(0, SPREAD, 16):
                level = [
                    level_row_table[slot * root_count + at, pl.ds(piece, 16), pl.ds(block * LANES, LANES)]
                    for at in (root, root + 1)
                ]
                for place in chosen:
                    if place * 16 % SPREAD != piece:
                        continue
                    col = levels_col[pl.ds(place * 16, 16), :]
                    dens = [col + row for row in level]
                    if (place * 16 // SPREAD + block) % 4 < PAIRED:
                        both = 1.0 / (dens[0] * dens[1])
                        values = [both * dens[1], both * dens[0]]
                    else:
                        values = [1.0 / den for den in dens]
                    for at, value in enumerate(values):
                        recip[slot, (root + at) * width_blocks + block, place] = value.astype(BF16)

    def recip_pair(slot, root):
        return jnp.concatenate(
            [recip[slot, root * width_blocks + at].reshape(virt, LANES) for at in range(2 * width_blocks)], axis=1
        )

    def mix(rows_pair, target):
        pair = jnp.concatenate([ints[row] for row in rows_pair], axis=1)
        both = jnp.dot(couple_ref[...], pair, preferred_element_type=F32)
        target[0] = both[:, :virt]
        target[1] = both[:, virt:]

    index = lax.broadcasted_iota(jnp.int32, (rows, virt), 0)
    low_bit = index % occ_domain == 0
    own_side = (index // occ_domain) % 2 == 0
    high_bit = index // terms == 0

    def pick(mask, values):
        return jnp.where(mask, jnp.broadcast_to(values[0], (rows, virt)), jnp.broadcast_to(values[1], (rows, virt)))

    def trial_terms(relative, root):
        return pick(
            low_bit, [trial_f32[relative, pl.ds(own * root_count + root, 1), :] for own in range(occ_domain)]
        )

    own_terms, lefts = [], {}

    def ready_own():
        scalars[-1].wait()
        pltpu.make_async_copy(trial_hbm.at[pl.ds(0, span * occ_domain)], trial, trial_sem).wait()
        for relative in range(span):
            for own in range(occ_domain):
                trial_f32[relative, pl.ds(own * root_count, root_count), :] = trial[
                    relative * occ_domain + own
                ].astype(F32)
        couple_ref[...] = jnp.concatenate([couple[row].astype(F32) for row in range(slab_rows)], axis=0).astype(BF16)
        own_copy.wait()
        for row in range(0, occ_domain, 2):
            mix((row, row + 1), mixed_own.at[pl.ds(row, 2)])
        own_terms.extend(trial_terms(0, root) for root in range(root_count))

    def lefts_of(slot):
        relative, first, second, energy = slots[slot]
        mix_first = [mixed_own[first, pl.ds(second * occ_domain + own, 1), :] for own in range(occ_domain)]
        first_terms = pick(low_bit, mix_first)
        left = [jnp.where(own_side, own_terms[root], first_terms) for root in range(root_count)]
        lefts[slot] = left, pick(high_bit, mix_first) * row_scale

    def multiply(slot, root):
        if root == 0:
            lefts_of(slot)
        left, first_by = lefts[slot]
        both = jnp.dot(
            jnp.concatenate([left[at] * first_by for at in (root, root + 1)], axis=0).astype(BF16),
            recip_pair(slot, root),
            preferred_element_type=F32,
        )
        product[slot, root] = both[:rows, :virt]
        product[slot, root + 1] = both[rows:, virt:]

    for step in ORDER:
        kind, at = step[0], step[1:]
        if kind == "R":
            slot, root = int(at[0]), 2 * int(at[1])
            if root == 0 and at[2:] != "b":
                fill_levels(slot)
            half = places * 2 // 3
            fill_recip(slot, root, {"": range(places), "a": range(half), "b": range(half, places)}[at[2:]])
        elif step == "Wo":
            ready_own()
        elif step == "Wf":
            far_copy.wait()
        elif step == "Mf":
            for slot in range(0, slot_count, 2):
                mix((slots[slot][2], slots[slot + 1][2]), mixed_far.at[pl.ds(slot, 2)])
        elif kind == "D":
            multiply(int(at[0]), 2 * int(at[1]))

    live_slots = pair_count[me]
    totals = [jnp.zeros((rows, virt), F32) for _ in range(span)]
    kept = []
    for slot, (relative, first, second, energy) in enumerate(slots):
        live = live_slots > slot
        mix_second = [
            mixed_far[slot, pl.ds(first * occ_domain + own, 1), :] for own in range(occ_domain)
        ]
        second_terms = pick(low_bit, mix_second)
        second_by = pick(high_bit, mix_second) * column_scale
        right = [jnp.where(own_side, second_terms, trial_terms(relative, root)) for root in range(root_count)]
        added = group_sums([product[slot, root] * right[root] for root in range(root_count)])
        for steps in range(1, span):
            totals[steps] += jnp.where(jnp.logical_and(live, relative == steps), added, 0.0)
        kept.append((lefts[slot][0], [value * second_by for value in right], live))

    for steps in range(1, span):
        stage[steps - 1] = totals[steps] * column_scale
    pl.semaphore_wait(barrier, 2 * (span - 1))
    for steps in range(1, span):
        copy = pltpu.make_async_remote_copy(
            src_ref=stage.at[steps - 1],
            dst_ref=landed.at[steps - 1],
            send_sem=send_sem,
            recv_sem=recv_sem,
            device_id={"aux": ahead(steps)},
            device_id_type=pl.DeviceIdType.MESH,
        )
        copy.start()

    result = totals[0]
    nothing = jnp.zeros((rows, virt), F32)
    for slot, (left, weights, live) in enumerate(kept):
        parts = []
        for root in range(0, root_count, 2):
            heads = [weights[at].astype(BF16).astype(F32) for at in (root, root + 1)]
            tails = [weights[at] - head for at, head in zip((root, root + 1), heads)]
            block = jnp.concatenate(
                [
                    jnp.concatenate([half[0], nothing] if at == 0 else [nothing, half[1]], axis=1)
                    for half in (heads, tails)
                    for at in (0, 1)
                ],
                axis=0,
            ).astype(BF16)
            both = lax.dot_general(
                block,
                recip_pair(slot, root),
                (((1,), (1,)), ((), ())),
                preferred_element_type=F32,
            )
            both = both[: 2 * rows] + both[2 * rows :]
            parts.append(both[:rows] * left[root])
            parts.append(both[rows:] * left[root + 1])
        result += jnp.where(live, group_sums(parts), 0.0)
    result = result * row_scale
    pltpu.make_async_copy(stage, landed, send_sem).wait()
    pltpu.make_async_copy(stage, landed, recv_sem).wait()
    for steps in range(1, span):
        result = result + landed[steps - 1]
    for own in range(occ_domain):
        out_ref[own] = result[own * root_count : (own + 1) * root_count]


def per_device(
    ints_ov, ints_oo, trial, occ_energy, vir_energy, root_shift, vir_blocks, pair_list, pair_count
):
    slab_rows, fitting, virt = ints_ov.shape
    occ_domain = ints_oo.shape[1]
    root_count = trial.shape[1]
    slot_count = pair_list.shape[1]
    span = slab_rows // occ_domain
    rows = occ_domain * root_count
    level_table = vir_energy.reshape(-1, LANES)
    blocks = vir_blocks.T
    pairs = pair_list.transpose(1, 2, 0)
    anywhere = pl.BlockSpec(memory_space=pl.ANY)
    return pl.pallas_call(
        functools.partial(
            sigma_kernel, lax.axis_size("aux"), span, slot_count, occ_domain, root_count
        ),
        out_shape=pltpu.VMEM((occ_domain, root_count, virt), F32),
        in_specs=[anywhere] * 9,
        out_specs=pl.BlockSpec(memory_space=pltpu.VMEM),
        scratch_shapes=[
            pltpu.VMEM(ints_ov.shape, BF16),
            pltpu.VMEM(ints_oo.shape, BF16),
            pltpu.VMEM((span * occ_domain, root_count, virt), BF16),
            pltpu.VMEM(level_table.shape, F32),
            pltpu.SMEM(occ_energy.shape, F32),
            pltpu.SMEM(root_shift.shape, F32),
            pltpu.SMEM(pair_count.shape, jnp.int32),
            pltpu.SMEM(blocks.shape, jnp.int32),
            pltpu.SMEM(pairs.shape, jnp.int32),
            pltpu.VMEM((virt, LANES), F32),
            pltpu.VMEM((slot_count * root_count, SPREAD, virt), F32),
            pltpu.VMEM((SPREAD, virt), F32),
            pltpu.VMEM((span, rows, virt), F32),
            pltpu.VMEM((occ_domain, slab_rows * occ_domain, virt), F32),
            pltpu.VMEM((slot_count, slab_rows * occ_domain, virt), F32),
            pltpu.VMEM((slab_rows * occ_domain, fitting), BF16),
            pltpu.VMEM((slot_count, root_count, rows, virt), F32),
            pltpu.VMEM((slot_count, root_count * virt // LANES, virt // 16, 16, LANES), BF16),
            pltpu.VMEM((span - 1, rows, virt), F32),
            pltpu.VMEM((span - 1, rows, virt), F32),
            pltpu.SemaphoreType.DMA((2,)),
            pltpu.SemaphoreType.DMA((8,)),
            pltpu.SemaphoreType.DMA,
            pltpu.SemaphoreType.DMA,
        ],
        compiler_params=pltpu.CompilerParams(collective_id=0, has_side_effects=True),
        name="sigma",
    )(ints_ov, ints_oo, trial, level_table, occ_energy, root_shift, pair_count, blocks, pairs)


def solution(mesh):
    in_specs = (
        P(("job", "aux"), None, None),
        P(("job", "aux"), None, None),
        P("job", None, None),
        P("job"),
        P("job"),
        P("job"),
        P("job", None),
        P("job", None, None),
        P("job"),
    )
    out_specs = P(("job", "aux"), None, None)
    return jax.shard_map(
        per_device, mesh=mesh, in_specs=in_specs, out_specs=out_specs, check_vma=False
    )
```

```python
import functools

import jax
import jax.numpy as jnp
from jax import lax
from jax.experimental import pallas as pl
from jax.experimental.pallas import tpu as pltpu
from jax.sharding import PartitionSpec as P

F32 = jnp.float32
BF16 = jnp.bfloat16
LANES = 128
PAIRED = 2
SPREAD = 32
ORDER = (
    "R00", "Wo", "R01", "D00", "D01", "R10", "R11", "D10",
    "D11", "R20", "R21", "D20", "D21", "R30", "Wf", "Mf",
    "R31", "D30", "D31",
)


def group_sums(parts):
    rows = parts[0].shape[0]
    index = lax.broadcasted_iota(jnp.int32, parts[0].shape, 0)
    step = 1
    while len(parts) > 1:
        low = (index // step) % 2 == 0
        parts = [
            jnp.where(low, even, pltpu.roll(odd, step, 0)) + jnp.where(low, pltpu.roll(even, rows - step, 0), odd)
            for even, odd in zip(parts[::2], parts[1::2])
        ]
        step *= 2
    return parts[0]


def sigma_kernel(
    ndomain, span, slot_count, occ_domain, root_count,
    ints_hbm, couple_hbm, trial_hbm, level_hbm, occ_hbm, shift_hbm, count_hbm, blocks_hbm, pairs_hbm,
    out_ref,
    ints, couple, trial, level_table, occ_energy, root_shift, pair_count, vir_blocks, pairs,
    levels_col, level_row_table, spread_ref, trial_f32, mixed_own, mixed_far, couple_ref, product, recip, stage, landed,
    ints_sem, small_sem, send_sem, recv_sem,
):
    me = lax.axis_index("aux")
    slab_rows, fitting, virt = ints.shape
    width_blocks = virt // LANES
    rows = occ_domain * root_count
    terms = 2 * occ_domain
    far_rows = slab_rows - occ_domain

    def ahead(steps):
        return lax.rem(me + steps, ndomain)

    scalars = [
        pltpu.make_async_copy(src, dst, small_sem.at[at])
        for at, (src, dst) in enumerate(
            [
                (level_hbm, level_table), (blocks_hbm, vir_blocks), (pairs_hbm, pairs), (occ_hbm, occ_energy),
                (shift_hbm, root_shift), (count_hbm, pair_count), (couple_hbm, couple),
            ]
        )
    ]
    for copy in scalars[:-1]:
        copy.start()
    own_copy = pltpu.make_async_copy(
        ints_hbm.at[pl.ds(0, occ_domain)], ints.at[pl.ds(0, occ_domain)], ints_sem.at[0]
    )
    far_copy = pltpu.make_async_copy(
        ints_hbm.at[pl.ds(occ_domain, far_rows)], ints.at[pl.ds(occ_domain, far_rows)], ints_sem.at[1]
    )
    own_copy.start()
    trial_sem = small_sem.at[7]
    for steps in range(span):
        pltpu.make_async_copy(
            trial_hbm.at[pl.ds(ahead(steps) * occ_domain, occ_domain)],
            trial.at[pl.ds(steps * occ_domain, occ_domain)],
            trial_sem,
        ).start()
    scalars[-1].start()
    far_copy.start()

    barrier = pltpu.get_barrier_semaphore()
    for steps in range(1, span):
        for other in (ahead(steps), ahead(ndomain - steps)):
            pl.semaphore_signal(
                barrier, inc=1, device_id={"aux": other}, device_id_type=pl.DeviceIdType.MESH
            )

    def factors(shape, axis, count):
        at = lax.broadcasted_iota(jnp.int32, shape, axis) % count
        return jnp.exp2(at.astype(F32) * (1.0 / count))

    spread = factors((SPREAD, virt), 0, SPREAD) * factors((SPREAD, virt), 1, LANES)
    spread_ref[...] = spread
    row_scale = factors((rows, virt), 1, SPREAD)
    column_scale = factors((rows, virt), 1, LANES)

    for copy in scalars[:-1]:
        copy.wait()

    def level_rows(relative):
        return [level_table[pl.ds(vir_blocks[block, ahead(relative)], 1), :] for block in range(width_blocks)]

    tall = jnp.concatenate([spread_ref[:, :LANES]] * (LANES // SPREAD), axis=0)
    for block, row in enumerate(level_rows(0)):
        levels_col[pl.ds(block * LANES, LANES), :] = jnp.broadcast_to(row, (LANES, LANES)).T * tall

    slots = []
    for slot in range(slot_count):
        occ_first = pairs[slot, 0, me]
        occ_second = pairs[slot, 1, me]
        relative = lax.rem(occ_second // occ_domain - me + ndomain, ndomain)
        relative = jnp.maximum(jnp.minimum(relative, span - 1), 1)
        first = lax.rem(occ_first, occ_domain)
        second = relative * occ_domain + lax.rem(occ_second, occ_domain)
        slots.append((relative, first, second, occ_energy[occ_first] + occ_energy[occ_second]))

    def fill_levels(slot):
        relative, first, second, energy = slots[slot]
        level_row = jnp.concatenate(level_rows(relative), axis=1) - energy
        for root in range(root_count):
            level_row_table[slot * root_count + root] = (level_row - root_shift[root]) * spread_ref[...]

    places = virt // 16

    def fill_recip(slot, root, chosen):
        for block in range(width_blocks):
            for piece in range(0, SPREAD, 16):
                level = [
                    level_row_table[slot * root_count + at, pl.ds(piece, 16), pl.ds(block * LANES, LANES)]
                    for at in (root, root + 1)
                ]
                for place in chosen:
                    if place * 16 % SPREAD != piece:
                        continue
                    col = levels_col[pl.ds(place * 16, 16), :]
                    dens = [col + row for row in level]
                    if (place * 16 // SPREAD + block) % 4 < PAIRED:
                        both = 1.0 / (dens[0] * dens[1])
                        values = [both * dens[1], both * dens[0]]
                    else:
                        values = [1.0 / den for den in dens]
                    for at, value in enumerate(values):
                        recip[slot, (root + at) * width_blocks + block, place] = value.astype(BF16)

    def recip_pair(slot, root):
        return jnp.concatenate(
            [recip[slot, root * width_blocks + at].reshape(virt, LANES) for at in range(2 * width_blocks)], axis=1
        )

    def mix(rows_pair, target):
        pair = jnp.concatenate([ints[row] for row in rows_pair], axis=1)
        both = jnp.dot(couple_ref[...], pair, preferred_element_type=F32)
        target[0] = both[:, :virt]
        target[1] = both[:, virt:]

    index = lax.broadcasted_iota(jnp.int32, (rows, virt), 0)
    low_bit = index % occ_domain == 0
    own_side = (index // occ_domain) % 2 == 0
    high_bit = index // terms == 0

    def pick(mask, values):
        return jnp.where(mask, jnp.broadcast_to(values[0], (rows, virt)), jnp.broadcast_to(values[1], (rows, virt)))

    def trial_terms(relative, root):
        return pick(
            low_bit, [trial_f32[relative, pl.ds(own * root_count + root, 1), :] for own in range(occ_domain)]
        )

    own_terms, lefts = [], {}

    def ready_own():
        scalars[-1].wait()
        pltpu.make_async_copy(trial_hbm.at[pl.ds(0, span * occ_domain)], trial, trial_sem).wait()
        for relative in range(span):
            for own in range(occ_domain):
                trial_f32[relative, pl.ds(own * root_count, root_count), :] = trial[
                    relative * occ_domain + own
                ].astype(F32)
        couple_ref[...] = jnp.concatenate([couple[row].astype(F32) for row in range(slab_rows)], axis=0).astype(BF16)
        own_copy.wait()
        for row in range(0, occ_domain, 2):
            mix((row, row + 1), mixed_own.at[pl.ds(row, 2)])
        own_terms.extend(trial_terms(0, root) for root in range(root_count))

    def lefts_of(slot):
        relative, first, second, energy = slots[slot]
        mix_first = [mixed_own[first, pl.ds(second * occ_domain + own, 1), :] for own in range(occ_domain)]
        first_terms = pick(low_bit, mix_first)
        left = [jnp.where(own_side, own_terms[root], first_terms) for root in range(root_count)]
        lefts[slot] = left, pick(high_bit, mix_first) * row_scale

    def multiply(slot, root):
        if root == 0:
            lefts_of(slot)
        left, first_by = lefts[slot]
        both = jnp.dot(
            jnp.concatenate([left[at] * first_by for at in (root, root + 1)], axis=0).astype(BF16),
            recip_pair(slot, root),
            preferred_element_type=F32,
        )
        product[slot, root] = both[:rows, :virt]
        product[slot, root + 1] = both[rows:, virt:]

    for step in ORDER:
        kind, at = step[0], step[1:]
        if kind == "R":
            slot, root = int(at[0]), 2 * int(at[1])
            if root == 0 and at[2:] != "b":
                fill_levels(slot)
            half = places * 2 // 3
            fill_recip(slot, root, {"": range(places), "a": range(half), "b": range(half, places)}[at[2:]])
        elif step == "Wo":
            ready_own()
        elif step == "Wf":
            far_copy.wait()
        elif step == "Mf":
            for slot in range(0, slot_count, 2):
                mix((slots[slot][2], slots[slot + 1][2]), mixed_far.at[pl.ds(slot, 2)])
        elif kind == "D":
            multiply(int(at[0]), 2 * int(at[1]))

    live_slots = pair_count[me]
    totals = [jnp.zeros((rows, virt), F32) for _ in range(span)]
    kept = []
    for slot, (relative, first, second, energy) in enumerate(slots):
        live = live_slots > slot
        mix_second = [
            mixed_far[slot, pl.ds(first * occ_domain + own, 1), :] for own in range(occ_domain)
        ]
        second_terms = pick(low_bit, mix_second)
        second_by = pick(high_bit, mix_second) * column_scale
        right = [jnp.where(own_side, second_terms, trial_terms(relative, root)) for root in range(root_count)]
        added = group_sums([product[slot, root] * right[root] for root in range(root_count)])
        for steps in range(1, span):
            totals[steps] += jnp.where(jnp.logical_and(live, relative == steps), added, 0.0)
        kept.append((lefts[slot][0], [value * second_by for value in right], live))

    pl.semaphore_wait(barrier, 2 * (span - 1))
    for steps in sorted(range(1, span), key=lambda steps: (steps == 1, steps)):
        stage[steps - 1] = totals[steps] * column_scale
        copy = pltpu.make_async_remote_copy(
            src_ref=stage.at[steps - 1],
            dst_ref=landed.at[steps - 1],
            send_sem=send_sem,
            recv_sem=recv_sem,
            device_id={"aux": ahead(steps)},
            device_id_type=pl.DeviceIdType.MESH,
        )
        copy.start()

    result = totals[0]
    nothing = jnp.zeros((rows, virt), F32)
    for slot, (left, weights, live) in enumerate(kept):
        parts = []
        for root in range(0, root_count, 2):
            heads = [weights[at].astype(BF16).astype(F32) for at in (root, root + 1)]
            tails = [weights[at] - head for at, head in zip((root, root + 1), heads)]
            block = jnp.concatenate(
                [
                    jnp.concatenate([half[0], nothing] if at == 0 else [nothing, half[1]], axis=1)
                    for half in (heads, tails)
                    for at in (0, 1)
                ],
                axis=0,
            ).astype(BF16)
            both = lax.dot_general(
                block,
                recip_pair(slot, root),
                (((1,), (1,)), ((), ())),
                preferred_element_type=F32,
            )
            both = both[: 2 * rows] + both[2 * rows :]
            parts.append(both[:rows] * left[root])
            parts.append(both[rows:] * left[root + 1])
        result += jnp.where(live, group_sums(parts), 0.0)
    result = result * row_scale
    pltpu.make_async_copy(stage, landed, send_sem).wait()
    pltpu.make_async_copy(stage, landed, recv_sem).wait()
    for steps in range(1, span):
        result = result + landed[steps - 1]
    for own in range(occ_domain):
        out_ref[own] = result[own * root_count : (own + 1) * root_count]


def per_device(
    ints_ov, ints_oo, trial, occ_energy, vir_energy, root_shift, vir_blocks, pair_list, pair_count
):
    slab_rows, fitting, virt = ints_ov.shape
    occ_domain = ints_oo.shape[1]
    root_count = trial.shape[1]
    slot_count = pair_list.shape[1]
    span = slab_rows // occ_domain
    rows = occ_domain * root_count
    level_table = vir_energy.reshape(-1, LANES)
    blocks = vir_blocks.T
    pairs = pair_list.transpose(1, 2, 0)
    anywhere = pl.BlockSpec(memory_space=pl.ANY)
    return pl.pallas_call(
        functools.partial(
            sigma_kernel, lax.axis_size("aux"), span, slot_count, occ_domain, root_count
        ),
        out_shape=pltpu.VMEM((occ_domain, root_count, virt), F32),
        in_specs=[anywhere] * 9,
        out_specs=pl.BlockSpec(memory_space=pltpu.VMEM),
        scratch_shapes=[
            pltpu.VMEM(ints_ov.shape, BF16),
            pltpu.VMEM(ints_oo.shape, BF16),
            pltpu.VMEM((span * occ_domain, root_count, virt), BF16),
            pltpu.VMEM(level_table.shape, F32),
            pltpu.SMEM(occ_energy.shape, F32),
            pltpu.SMEM(root_shift.shape, F32),
            pltpu.SMEM(pair_count.shape, jnp.int32),
            pltpu.SMEM(blocks.shape, jnp.int32),
            pltpu.SMEM(pairs.shape, jnp.int32),
            pltpu.VMEM((virt, LANES), F32),
            pltpu.VMEM((slot_count * root_count, SPREAD, virt), F32),
            pltpu.VMEM((SPREAD, virt), F32),
            pltpu.VMEM((span, rows, virt), F32),
            pltpu.VMEM((occ_domain, slab_rows * occ_domain, virt), F32),
            pltpu.VMEM((slot_count, slab_rows * occ_domain, virt), F32),
            pltpu.VMEM((slab_rows * occ_domain, fitting), BF16),
            pltpu.VMEM((slot_count, root_count, rows, virt), F32),
            pltpu.VMEM((slot_count, root_count * virt // LANES, virt // 16, 16, LANES), BF16),
            pltpu.VMEM((span - 1, rows, virt), F32),
            pltpu.VMEM((span - 1, rows, virt), F32),
            pltpu.SemaphoreType.DMA((2,)),
            pltpu.SemaphoreType.DMA((8,)),
            pltpu.SemaphoreType.DMA,
            pltpu.SemaphoreType.DMA,
        ],
        compiler_params=pltpu.CompilerParams(collective_id=0, has_side_effects=True),
        name="sigma",
    )(ints_ov, ints_oo, trial, level_table, occ_energy, root_shift, pair_count, blocks, pairs)


def solution(mesh):
    in_specs = (
        P(("job", "aux"), None, None),
        P(("job", "aux"), None, None),
        P("job", None, None),
        P("job"),
        P("job"),
        P("job"),
        P("job", None),
        P("job", None, None),
        P("job"),
    )
    out_specs = P(("job", "aux"), None, None)
    return jax.shard_map(
        per_device, mesh=mesh, in_specs=in_specs, out_specs=out_specs, check_vma=False
    )
```

```python
import functools

import jax
import jax.numpy as jnp
from jax import lax
from jax.experimental import pallas as pl
from jax.experimental.pallas import tpu as pltpu
from jax.sharding import PartitionSpec as P

F32 = jnp.float32
BF16 = jnp.bfloat16
LANES = 128
PAIRED = 2
SPREAD = 32
ORDER = (
    "R00", "Wo", "R01", "D00", "D01", "R10", "R11", "D10",
    "D11", "R20", "R21", "D20", "D21", "R30", "Wf", "Mf",
    "R31", "D30", "D31",
)


def group_sums(parts):
    rows = parts[0].shape[0]
    index = lax.broadcasted_iota(jnp.int32, parts[0].shape, 0)
    step = 1
    while len(parts) > 1:
        low = (index // step) % 2 == 0
        parts = [
            jnp.where(low, even, pltpu.roll(odd, step, 0)) + jnp.where(low, pltpu.roll(even, rows - step, 0), odd)
            for even, odd in zip(parts[::2], parts[1::2])
        ]
        step *= 2
    return parts[0]


def sigma_kernel(
    ndomain, span, slot_count, occ_domain, root_count,
    ints_hbm, couple_hbm, trial_hbm, level_hbm, occ_hbm, shift_hbm, count_hbm, blocks_hbm, pairs_hbm,
    out_ref,
    ints, couple, trial, level_table, occ_energy, root_shift, pair_count, vir_blocks, pairs,
    levels_col, level_row_table, spread_ref, trial_f32, mixed_own, mixed_far, couple_ref, product, recip, stage, landed,
    ints_sem, small_sem, send_sem, recv_sem,
):
    me = lax.axis_index("aux")
    slab_rows, fitting, virt = ints.shape
    width_blocks = virt // LANES
    rows = occ_domain * root_count
    terms = 2 * occ_domain
    far_rows = slab_rows - occ_domain

    def ahead(steps):
        return lax.rem(me + steps, ndomain)

    scalars = [
        pltpu.make_async_copy(src, dst, small_sem.at[at])
        for at, (src, dst) in enumerate(
            [
                (level_hbm, level_table), (blocks_hbm, vir_blocks), (pairs_hbm, pairs), (occ_hbm, occ_energy),
                (shift_hbm, root_shift), (count_hbm, pair_count), (couple_hbm, couple),
            ]
        )
    ]
    for copy in scalars[:-1]:
        copy.start()
    own_copy = pltpu.make_async_copy(
        ints_hbm.at[pl.ds(0, occ_domain)], ints.at[pl.ds(0, occ_domain)], ints_sem.at[0]
    )
    far_copy = pltpu.make_async_copy(
        ints_hbm.at[pl.ds(occ_domain, far_rows)], ints.at[pl.ds(occ_domain, far_rows)], ints_sem.at[1]
    )
    own_copy.start(priority=1)
    trial_sem = small_sem.at[7]
    for steps in range(span):
        pltpu.make_async_copy(
            trial_hbm.at[pl.ds(ahead(steps) * occ_domain, occ_domain)],
            trial.at[pl.ds(steps * occ_domain, occ_domain)],
            trial_sem,
        ).start()
    scalars[-1].start()
    far_copy.start(priority=1)

    barrier = pltpu.get_barrier_semaphore()
    for steps in range(1, span):
        for other in (ahead(steps), ahead(ndomain - steps)):
            pl.semaphore_signal(
                barrier, inc=1, device_id={"aux": other}, device_id_type=pl.DeviceIdType.MESH
            )

    def factors(shape, axis, count):
        at = lax.broadcasted_iota(jnp.int32, shape, axis) % count
        return jnp.exp2(at.astype(F32) * (1.0 / count))

    spread = factors((SPREAD, virt), 0, SPREAD) * factors((SPREAD, virt), 1, LANES)
    spread_ref[...] = spread
    row_scale = factors((rows, virt), 1, SPREAD)
    column_scale = factors((rows, virt), 1, LANES)

    for copy in scalars[:-1]:
        copy.wait()

    def level_rows(relative):
        return [level_table[pl.ds(vir_blocks[block, ahead(relative)], 1), :] for block in range(width_blocks)]

    tall = jnp.concatenate([spread_ref[:, :LANES]] * (LANES // SPREAD), axis=0)
    for block, row in enumerate(level_rows(0)):
        levels_col[pl.ds(block * LANES, LANES), :] = jnp.broadcast_to(row, (LANES, LANES)).T * tall

    slots = []
    for slot in range(slot_count):
        occ_first = pairs[slot, 0, me]
        occ_second = pairs[slot, 1, me]
        relative = lax.rem(occ_second // occ_domain - me + ndomain, ndomain)
        relative = jnp.maximum(jnp.minimum(relative, span - 1), 1)
        first = lax.rem(occ_first, occ_domain)
        second = relative * occ_domain + lax.rem(occ_second, occ_domain)
        slots.append((relative, first, second, occ_energy[occ_first] + occ_energy[occ_second]))

    def fill_levels(slot):
        relative, first, second, energy = slots[slot]
        level_row = jnp.concatenate(level_rows(relative), axis=1) - energy
        for root in range(root_count):
            level_row_table[slot * root_count + root] = (level_row - root_shift[root]) * spread_ref[...]

    places = virt // 16

    def fill_recip(slot, root, chosen):
        for block in range(width_blocks):
            for piece in range(0, SPREAD, 16):
                level = [
                    level_row_table[slot * root_count + at, pl.ds(piece, 16), pl.ds(block * LANES, LANES)]
                    for at in (root, root + 1)
                ]
                for place in chosen:
                    if place * 16 % SPREAD != piece:
                        continue
                    col = levels_col[pl.ds(place * 16, 16), :]
                    dens = [col + row for row in level]
                    if (place * 16 // SPREAD + block) % 4 < PAIRED:
                        both = 1.0 / (dens[0] * dens[1])
                        values = [both * dens[1], both * dens[0]]
                    else:
                        values = [1.0 / den for den in dens]
                    for at, value in enumerate(values):
                        recip[slot, (root + at) * width_blocks + block, place] = value.astype(BF16)

    def recip_pair(slot, root):
        return jnp.concatenate(
            [recip[slot, root * width_blocks + at].reshape(virt, LANES) for at in range(2 * width_blocks)], axis=1
        )

    def mix(rows_pair, target):
        pair = jnp.concatenate([ints[row] for row in rows_pair], axis=1)
        both = jnp.dot(couple_ref[...], pair, preferred_element_type=F32)
        target[0] = both[:, :virt]
        target[1] = both[:, virt:]

    index = lax.broadcasted_iota(jnp.int32, (rows, virt), 0)
    low_bit = index % occ_domain == 0
    own_side = (index // occ_domain) % 2 == 0
    high_bit = index // terms == 0

    def pick(mask, values):
        return jnp.where(mask, jnp.broadcast_to(values[0], (rows, virt)), jnp.broadcast_to(values[1], (rows, virt)))

    def trial_terms(relative, root):
        return pick(
            low_bit, [trial_f32[relative, pl.ds(own * root_count + root, 1), :] for own in range(occ_domain)]
        )

    own_terms, lefts = [], {}

    def ready_own():
        scalars[-1].wait()
        pltpu.make_async_copy(trial_hbm.at[pl.ds(0, span * occ_domain)], trial, trial_sem).wait()
        for relative in range(span):
            for own in range(occ_domain):
                trial_f32[relative, pl.ds(own * root_count, root_count), :] = trial[
                    relative * occ_domain + own
                ].astype(F32)
        couple_ref[...] = jnp.concatenate([couple[row].astype(F32) for row in range(slab_rows)], axis=0).astype(BF16)
        own_copy.wait()
        for row in range(0, occ_domain, 2):
            mix((row, row + 1), mixed_own.at[pl.ds(row, 2)])
        own_terms.extend(trial_terms(0, root) for root in range(root_count))

    def lefts_of(slot):
        relative, first, second, energy = slots[slot]
        mix_first = [mixed_own[first, pl.ds(second * occ_domain + own, 1), :] for own in range(occ_domain)]
        first_terms = pick(low_bit, mix_first)
        left = [jnp.where(own_side, own_terms[root], first_terms) for root in range(root_count)]
        lefts[slot] = left, pick(high_bit, mix_first) * row_scale

    def multiply(slot, root):
        if root == 0:
            lefts_of(slot)
        left, first_by = lefts[slot]
        both = jnp.dot(
            jnp.concatenate([left[at] * first_by for at in (root, root + 1)], axis=0).astype(BF16),
            recip_pair(slot, root),
            preferred_element_type=F32,
        )
        product[slot, root] = both[:rows, :virt]
        product[slot, root + 1] = both[rows:, virt:]

    for step in ORDER:
        kind, at = step[0], step[1:]
        if kind == "R":
            slot, root = int(at[0]), 2 * int(at[1])
            if root == 0 and at[2:] != "b":
                fill_levels(slot)
            half = places * 2 // 3
            fill_recip(slot, root, {"": range(places), "a": range(half), "b": range(half, places)}[at[2:]])
        elif step == "Wo":
            ready_own()
        elif step == "Wf":
            far_copy.wait()
        elif step == "Mf":
            for slot in range(0, slot_count, 2):
                mix((slots[slot][2], slots[slot + 1][2]), mixed_far.at[pl.ds(slot, 2)])
        elif kind == "D":
            multiply(int(at[0]), 2 * int(at[1]))

    live_slots = pair_count[me]
    totals = [jnp.zeros((rows, virt), F32) for _ in range(span)]
    kept = []
    for slot, (relative, first, second, energy) in enumerate(slots):
        live = live_slots > slot
        mix_second = [
            mixed_far[slot, pl.ds(first * occ_domain + own, 1), :] for own in range(occ_domain)
        ]
        second_terms = pick(low_bit, mix_second)
        second_by = pick(high_bit, mix_second) * column_scale
        right = [jnp.where(own_side, second_terms, trial_terms(relative, root)) for root in range(root_count)]
        added = group_sums([product[slot, root] * right[root] for root in range(root_count)])
        for steps in range(1, span):
            totals[steps] += jnp.where(jnp.logical_and(live, relative == steps), added, 0.0)
        kept.append((lefts[slot][0], [value * second_by for value in right], live))

    pl.semaphore_wait(barrier, 2 * (span - 1))
    for steps in sorted(range(1, span), key=lambda steps: (steps == 1, steps)):
        stage[steps - 1] = totals[steps] * column_scale
        copy = pltpu.make_async_remote_copy(
            src_ref=stage.at[steps - 1],
            dst_ref=landed.at[steps - 1],
            send_sem=send_sem,
            recv_sem=recv_sem,
            device_id={"aux": ahead(steps)},
            device_id_type=pl.DeviceIdType.MESH,
        )
        copy.start()

    result = totals[0]
    nothing = jnp.zeros((rows, virt), F32)
    for slot, (left, weights, live) in enumerate(kept):
        parts = []
        for root in range(0, root_count, 2):
            heads = [weights[at].astype(BF16).astype(F32) for at in (root, root + 1)]
            tails = [weights[at] - head for at, head in zip((root, root + 1), heads)]
            block = jnp.concatenate(
                [
                    jnp.concatenate([half[0], nothing] if at == 0 else [nothing, half[1]], axis=1)
                    for half in (heads, tails)
                    for at in (0, 1)
                ],
                axis=0,
            ).astype(BF16)
            both = lax.dot_general(
                block,
                recip_pair(slot, root),
                (((1,), (1,)), ((), ())),
                preferred_element_type=F32,
            )
            both = both[: 2 * rows] + both[2 * rows :]
            parts.append(both[:rows] * left[root])
            parts.append(both[rows:] * left[root + 1])
        result += jnp.where(live, group_sums(parts), 0.0)
    result = result * row_scale
    pltpu.make_async_copy(stage, landed, send_sem).wait()
    pltpu.make_async_copy(stage, landed, recv_sem).wait()
    for steps in range(1, span):
        result = result + landed[steps - 1]
    for own in range(occ_domain):
        out_ref[own] = result[own * root_count : (own + 1) * root_count]


def per_device(
    ints_ov, ints_oo, trial, occ_energy, vir_energy, root_shift, vir_blocks, pair_list, pair_count
):
    slab_rows, fitting, virt = ints_ov.shape
    occ_domain = ints_oo.shape[1]
    root_count = trial.shape[1]
    slot_count = pair_list.shape[1]
    span = slab_rows // occ_domain
    rows = occ_domain * root_count
    level_table = vir_energy.reshape(-1, LANES)
    blocks = vir_blocks.T
    pairs = pair_list.transpose(1, 2, 0)
    anywhere = pl.BlockSpec(memory_space=pl.ANY)
    return pl.pallas_call(
        functools.partial(
            sigma_kernel, lax.axis_size("aux"), span, slot_count, occ_domain, root_count
        ),
        out_shape=pltpu.VMEM((occ_domain, root_count, virt), F32),
        in_specs=[anywhere] * 9,
        out_specs=pl.BlockSpec(memory_space=pltpu.VMEM),
        scratch_shapes=[
            pltpu.VMEM(ints_ov.shape, BF16),
            pltpu.VMEM(ints_oo.shape, BF16),
            pltpu.VMEM((span * occ_domain, root_count, virt), BF16),
            pltpu.VMEM(level_table.shape, F32),
            pltpu.SMEM(occ_energy.shape, F32),
            pltpu.SMEM(root_shift.shape, F32),
            pltpu.SMEM(pair_count.shape, jnp.int32),
            pltpu.SMEM(blocks.shape, jnp.int32),
            pltpu.SMEM(pairs.shape, jnp.int32),
            pltpu.VMEM((virt, LANES), F32),
            pltpu.VMEM((slot_count * root_count, SPREAD, virt), F32),
            pltpu.VMEM((SPREAD, virt), F32),
            pltpu.VMEM((span, rows, virt), F32),
            pltpu.VMEM((occ_domain, slab_rows * occ_domain, virt), F32),
            pltpu.VMEM((slot_count, slab_rows * occ_domain, virt), F32),
            pltpu.VMEM((slab_rows * occ_domain, fitting), BF16),
            pltpu.VMEM((slot_count, root_count, rows, virt), F32),
            pltpu.VMEM((slot_count, root_count * virt // LANES, virt // 16, 16, LANES), BF16),
            pltpu.VMEM((span - 1, rows, virt), F32),
            pltpu.VMEM((span - 1, rows, virt), F32),
            pltpu.SemaphoreType.DMA((2,)),
            pltpu.SemaphoreType.DMA((8,)),
            pltpu.SemaphoreType.DMA,
            pltpu.SemaphoreType.DMA,
        ],
        compiler_params=pltpu.CompilerParams(collective_id=0, has_side_effects=True),
        name="sigma",
    )(ints_ov, ints_oo, trial, level_table, occ_energy, root_shift, pair_count, blocks, pairs)


def solution(mesh):
    in_specs = (
        P(("job", "aux"), None, None),
        P(("job", "aux"), None, None),
        P("job", None, None),
        P("job"),
        P("job"),
        P("job"),
        P("job", None),
        P("job", None, None),
        P("job"),
    )
    out_specs = P(("job", "aux"), None, None)
    return jax.shard_map(
        per_device, mesh=mesh, in_specs=in_specs, out_specs=out_specs, check_vma=False
    )
```
